32 devices in a mesh: batch: 1 (over z), col: 4 (over y), row: 8 (over x, core).
Axes of the slice: x: 4, y: 4, z: 1, core: 2. Of those that a mesh axis runs over, the one named last changes fastest.
The devices are a block of a 4x4x8 slice.
Arguments:
- lower_tri: float32 [3072, 3072], P(('batch', 'row'), 'col')
Outputs:
- output: float32 [3072, 3072], P(('batch', 'row'), 'col')
All inputs are finite; a program needn't handle non-finite values.
Results may differ from the reference program's by a relative error of at most 0.001.
Values sent between devices are 32-bit elements.
A program may use at most 768 MiB of HBM per device.

```python
import jax
import jax.numpy as jnp
from jax import lax

N = 3072
DEPTH = 3
HIGHEST = lax.Precision.HIGHEST


def setup_inputs(seed: int = 0, part: int = 0) -> dict:
    base_key = jax.random.fold_in(jax.random.key(seed), part)
    key_off, key_diag = jax.random.split(base_key)
    entries = jax.random.normal(key_off, (N, N), jnp.float32) * (N ** -0.5)
    diag_vals = jax.random.uniform(key_diag, (N,), jnp.float32, 2.0, 4.0)
    lower_tri = jnp.tril(entries, -1) + jnp.diag(diag_vals)
    return {"lower_tri": lower_tri}


def invert_lower(sub_block, depth_n):
    full_size = sub_block.shape[0]
    if depth_n == 0:
        unit_mat = jnp.eye(full_size, dtype=jnp.float32)
        return lax.linalg.triangular_solve(sub_block, unit_mat, left_side=True, lower=True)
    half_size = full_size // 2
    inv_a = invert_lower(sub_block[:half_size, :half_size], depth_n - 1)
    inv_b = invert_lower(sub_block[half_size:, half_size:], depth_n - 1)
    low_c = sub_block[half_size:, :half_size]
    prod_t = jnp.dot(low_c, inv_a, precision=HIGHEST, preferred_element_type=jnp.float32)
    low_x = -jnp.dot(inv_b, prod_t, precision=HIGHEST, preferred_element_type=jnp.float32)
    top_half = jnp.concatenate([inv_a, jnp.zeros_like(inv_a)], axis=1)
    bottom = jnp.concatenate([low_x, inv_b], axis=1)
    return jnp.concatenate([top_half, bottom], axis=0)


def reference(lower_tri):
    inv_l = invert_lower(lower_tri, DEPTH)
    contract_dims = (((0,), (0,)), ((), ()))
    return lax.dot_general(inv_l, inv_l, contract_dims, precision=HIGHEST, preferred_element_type=jnp.float32)
```

```python
import jax
import jax.numpy as jnp
from jax import lax
from jax.experimental import pallas as pl
from jax.experimental.pallas import tpu as pltpu
from jax.sharding import PartitionSpec as P

HIGHEST = lax.Precision.HIGHEST
MESH = pl.DeviceIdType.MESH
SIDE = 4


def dot_nn(a, b):
    return lax.dot_general(a, b, (((1,), (0,)), ((), ())), precision=HIGHEST, preferred_element_type=jnp.float32)


def dot_nt(a, b):
    return lax.dot_general(a, b, (((1,), (1,)), ((), ())), precision=HIGHEST, preferred_element_type=jnp.float32)


def leaf_inverse(leaf, inv):
    order = leaf.shape[0]
    part = 128
    count = order // part
    rows = lax.broadcasted_iota(jnp.int32, (part, part), 0)
    cols = lax.broadcasted_iota(jnp.int32, (part, part), 1)

    def blk(i, j):
        return leaf[part * i : part * (i + 1), part * j : part * (j + 1)]

    diag = [blk(q, q) for q in range(count)]
    done = [jnp.where(rows == cols, 1.0 / d, 0.0) for d in diag]
    size = 1
    while size < part:
        low = (rows // (2 * size) == cols // (2 * size)) & (rows // size % 2 == 1) & (cols // size % 2 == 0)
        prods = [dot_nn(jnp.where(low, d, 0.0), x) for d, x in zip(diag, done)]
        done = [x - dot_nn(x, t) for x, t in zip(done, prods)]
        size *= 2
    out = {}
    for i in range(count):
        out[i, i] = done[i]
    for gap in range(1, count):
        for j in range(count - gap):
            i = j + gap
            acc = dot_nn(blk(i, j), out[j, j])
            for k in range(j + 1, i):
                acc = acc + dot_nn(blk(i, k), out[k, j])
            out[i, j] = -dot_nn(out[i, i], acc)
    for i in range(count):
        for j in range(count):
            val = out[i, j] if j <= i else jnp.zeros((part, part), jnp.float32)
            inv[part * i : part * (i + 1), part * j : part * (j + 1)] = val


def make_kernel(leaf_n, share, strip):
    wide = 2 * leaf_n
    shifts = (0, SIDE - 1, 1, 2)
    DIRS = (1, -1, 1, -1)

    def kernel(own, out, off1, off2, off3, diag, leaf, inv, pmat, zmat,
               scat_send, scat_recv, ring_send, ring_recv, pair_send, pair_recv, out_send, out_recv):
        row = lax.axis_index("row")
        y = lax.axis_index("col")
        x = row // 2
        k = row % 2
        me = SIDE * x + y
        offs = {1: off1, 2: off2, 3: off3}

        def dev(cx, cy, core):
            return {"row": 2 * cx + core, "col": cy}

        barrier = pltpu.get_barrier_semaphore()

        def greet(t, carry):
            @pl.when(t != row * SIDE + y)
            def _():
                pl.semaphore_signal(barrier, inc=1, device_id={"row": t // SIDE, "col": t % SIDE}, device_id_type=MESH)
            return carry

        lax.fori_loop(0, 2 * SIDE * SIDE, greet, 0)
        pl.semaphore_wait(barrier, 2 * SIDE * SIDE - 1)

        def scatter(src_of, dst_of, cond, core, send_row, sem, phase):
            @pl.when(cond)
            def _():
                def body(m, carry):
                    src = src_of(pl.multiple_of(strip * m, 8))
                    dst = dst_of(pl.multiple_of(strip * m, 8))
                    here = (m == me) & (core == k)

                    @pl.when(here)
                    def _():
                        c = pltpu.make_async_copy(src, dst, scat_recv.at[sem])
                        if phase == 0:
                            c.start()

                    @pl.when(jnp.logical_not(here))
                    def _():
                        c = pltpu.make_async_remote_copy(
                            src_ref=src, dst_ref=dst, send_sem=scat_send.at[send_row, m], recv_sem=scat_recv.at[sem],
                            device_id=dev(m // SIDE, m % SIDE, core), device_id_type=MESH)
                        if phase == 0:
                            c.start()
                        else:
                            c.wait_send()
                    return carry

                lax.fori_loop(0, SIDE * SIDE, body, 0)

        def off_dst(a, yy):
            ybase = pl.multiple_of(wide * yy, 128)
            return lambda r: offs[a].at[pl.ds(pl.multiple_of(leaf_n * k, 8) + r, strip), pl.ds(ybase, wide)]

        def scatter_off(a, phase):
            for yy in range(a):
                scatter(lambda r: own.at[pl.ds(r, strip), :], off_dst(a, yy), (x == a) & (y == yy), k, 0,
                        a * (a - 1) // 2 + yy, phase)

        def scatter_low(a, phase):
            core = a // 2
            scatter(lambda r: own.at[pl.ds(r, strip), pl.ds(0, leaf_n)],
                    lambda r: diag.at[core, 4 + a % 2, pl.ds(r, strip), :],
                    (x == a) & (y == a) & (k == 1), core, 1, 10 + a % 2, phase)

        def scatter_inv(a, phase):
            scatter(lambda r: inv.at[pl.ds(r, strip), :],
                    lambda r: diag.at[k, a, pl.ds(r, strip), :],
                    (x == a) & (y == a), k, 0, 6 + a, phase)

        def landed(dst, src_like, sem, is_source):
            @pl.when(is_source)
            def _():
                pltpu.make_async_copy(src_like, dst, scat_recv.at[sem]).wait()

            @pl.when(jnp.logical_not(is_source))
            def _():
                pltpu.make_async_remote_copy(
                    src_ref=src_like, dst_ref=dst, send_sem=scat_send.at[0, 0], recv_sem=scat_recv.at[sem],
                    device_id=dev(x, y, 1 - k), device_id_type=MESH).wait_recv()

        mine = pl.multiple_of(strip * me, 8)

        def landed_off(a):
            for yy in range(a):
                landed(off_dst(a, yy)(mine), own.at[pl.ds(mine, strip), :], a * (a - 1) // 2 + yy, (x == a) & (y == yy))

        def landed_diag():
            for a in range(SIDE):
                landed(diag.at[k, a, pl.ds(mine, strip), :], inv.at[pl.ds(mine, strip), :], 6 + a, (x == a) & (y == a))
            for q in range(2):
                a = 2 * k + q
                landed(diag.at[k, 4 + q, pl.ds(mine, strip), :], inv.at[pl.ds(mine, strip), :], 10 + q,
                       (x == a) & (y == a) & (k == 1))

        def chip_at(core, du, dv):
            cx = (x + du + core * (dv - du)) % SIDE
            cy = (y + dv + core * (du - dv)) % SIDE
            return cx, cy

        def piece(rnd, core, cx, cy):
            r = pl.multiple_of(strip * (SIDE * cx + cy), 8)
            if rnd == 2:
                return diag.at[core, :, pl.ds(r, strip), :]
            ref = {0: off1, 1: off2, 3: off3}[rnd]
            return ref.at[pl.ds(pl.multiple_of(leaf_n * core, 8) + r, strip), :]

        pending = []

        def ring_copy(rnd, du, dv, tu, tv, idx):
            ref = piece(rnd, k, *chip_at(k, du, dv))
            return pltpu.make_async_remote_copy(
                src_ref=ref, dst_ref=ref, send_sem=ring_send.at[rnd, idx], recv_sem=ring_recv.at[rnd, idx],
                device_id=dev(*chip_at(k, tu, tv), k), device_id_type=MESH)

        def ring_start(*args):
            c = ring_copy(*args)
            c.start()
            pending.append(c)

        def ring_wait(rnd, du, dv, idx):
            ring_copy(rnd, du, dv, 0, 1, idx).wait_recv()

        def pair_copy(rnd, core, du, dv, idx):
            ref = piece(rnd, core, *chip_at(core, du, dv))
            return pltpu.make_async_remote_copy(
                src_ref=ref, dst_ref=ref, send_sem=pair_send.at[rnd, idx], recv_sem=pair_recv.at[rnd, idx],
                device_id=dev(x, y, 1 - k), device_id_type=MESH)

        def pair_start(rnd, g, dv):
            c = pair_copy(rnd, k, shifts[g], dv % SIDE, SIDE * g + dv % SIDE)
            c.start()
            pending.append(c)

        def spread(rnd, g):
            ring_start(rnd, shifts[g], 0, 0, 1, 3 + 3 * g)
            ring_start(rnd, shifts[g], 0, 0, -1, 4 + 3 * g)
            pair_start(rnd, g, 0)

        def first_axis(rnd):
            ring_start(rnd, 0, 0, 1, 0, 0)
            ring_start(rnd, 0, 0, -1, 0, 1)
            spread(rnd, 0)
            ring_wait(rnd, -1, 0, 0)
            if rnd % 2 == 0:
                ring_start(rnd, -1, 0, 1, 0, 2)
            spread(rnd, 1)
            ring_wait(rnd, 1, 0, 1)
            if rnd % 2 == 1:
                ring_start(rnd, 1, 0, -1, 0, 2)
            spread(rnd, 2)
            ring_wait(rnd, 2, 0, 2)
            spread(rnd, 3)

        def second_axis(rnd):
            for g in range(4):
                ring_wait(rnd, shifts[g], -1, 3 + 3 * g)
                if DIRS[g] == 1:
                    ring_start(rnd, shifts[g], -1, 0, 1, 5 + 3 * g)
                pair_start(rnd, g, -1)
                ring_wait(rnd, shifts[g], 1, 4 + 3 * g)
                if DIRS[g] == -1:
                    ring_start(rnd, shifts[g], 1, 0, -1, 5 + 3 * g)
                pair_start(rnd, g, 1)
            for g in range(4):
                ring_wait(rnd, shifts[g], 2, 5 + 3 * g)
                pair_start(rnd, g, 2)

        def pair_done(rnd):
            for g in range(4):
                for dv in range(SIDE):
                    pair_copy(rnd, 1 - k, shifts[g], dv, SIDE * g + dv).wait_recv()

        def low_of(a):
            return diag[a // 2, 4 + a % 2]

        def inv_of(i):
            return diag[i % 2, i // 2]

        j0 = leaf_n * row + share * y
        rowi = lax.broadcasted_iota(jnp.int32, (share, leaf_n), 0)
        coli = lax.broadcasted_iota(jnp.int32, (share, leaf_n), 1)

        def forward(a):
            lo, hi = wide * a, wide * a + leaf_n
            r0 = jnp.where(rowi + j0 == coli + lo, 1.0, 0.0)
            r1 = jnp.where(rowi + j0 == coli + hi, 1.0, 0.0)
            if a:
                acc = dot_nt(pmat[:, :lo], offs[a][...])
                r0 = r0 - acc[:, :leaf_n]
                r1 = r1 - acc[:, leaf_n:]
            p0 = dot_nt(r0, inv_of(2 * a))
            pmat[:, lo:hi] = p0
            pmat[:, hi : hi + leaf_n] = dot_nt(r1 - dot_nt(p0, low_of(a)), inv_of(2 * a + 1))

        def out_copy(i, yy, src_y):
            return pltpu.make_async_remote_copy(
                src_ref=zmat.at[:, leaf_n * i : leaf_n * (i + 1)],
                dst_ref=out.at[pl.ds(pl.multiple_of(share * src_y, 8), share), leaf_n * (i % 2) : leaf_n * (i % 2 + 1)],
                send_sem=out_send.at[i], recv_sem=out_recv.at[src_y, i % 2],
                device_id={"row": row, "col": yy}, device_id_type=MESH)

        def out_local(i):
            return pltpu.make_async_copy(
                zmat.at[:, leaf_n * i : leaf_n * (i + 1)],
                out.at[pl.ds(pl.multiple_of(share * y, 8), share), leaf_n * (i % 2) : leaf_n * (i % 2 + 1)],
                out_send.at[i])

        def ship(i, wait):
            @pl.when(y == i // 2)
            def _():
                c = out_local(i)
                c.wait() if wait else c.start()

            @pl.when(y != i // 2)
            def _():
                c = out_copy(i, i // 2, y)
                c.wait_send() if wait else c.start()

        def backward(a):
            lo, hi = wide * a, wide * a + leaf_n
            r0 = pmat[:, lo:hi]
            r1 = pmat[:, hi : hi + leaf_n]
            for b in range(a + 1, SIDE):
                acc = dot_nn(zmat[:, wide * b : wide * (b + 1)], offs[b][:, lo : lo + wide])
                r0 = r0 - acc[:, :leaf_n]
                r1 = r1 - acc[:, leaf_n:]
            z1 = dot_nn(r1, inv_of(2 * a + 1))
            zmat[:, hi : hi + leaf_n] = z1
            ship(2 * a + 1, False)
            zmat[:, lo:hi] = dot_nn(r0 - dot_nn(z1, low_of(a)), inv_of(2 * a))
            ship(2 * a, False)

        for a in range(1, SIDE):
            scatter_off(a, 0)
        for a in range(SIDE):
            scatter_low(a, 0)

        @pl.when((x == y) & (k == 0))
        def _():
            leaf[...] = own[:, :leaf_n]

        @pl.when((x == y) & (k == 1))
        def _():
            leaf[...] = own[:, leaf_n:]

        @pl.when(x == y)
        def _():
            leaf_inverse(leaf, inv)

        for a in range(SIDE):
            scatter_inv(a, 0)

        landed_off(1)
        first_axis(0)
        landed_off(2)
        first_axis(1)
        second_axis(0)
        landed_diag()
        first_axis(2)
        second_axis(1)
        landed_off(3)
        first_axis(3)
        second_axis(2)
        pair_done(0)
        pair_done(2)
        forward(0)
        forward(1)
        pair_done(1)
        forward(2)
        second_axis(3)
        pair_done(3)
        forward(3)
        for a in range(SIDE - 1, -1, -1):
            backward(a)

        for c in pending:
            c.wait_send()
        for a in range(1, SIDE):
            scatter_off(a, 1)
        for a in range(SIDE):
            scatter_low(a, 1)
            scatter_inv(a, 1)
        for i in range(2 * SIDE):
            ship(i, True)
        for yy in range(SIDE):
            @pl.when(y != yy)
            def _():
                for h in range(2):
                    out_copy(h, y, yy).wait_recv()

    return kernel


def solution(mesh):
    count_c = mesh.shape["col"]

    def local_fn(block):
        leaf_n, wide = block.shape
        share = leaf_n // count_c
        strip = leaf_n // (SIDE * SIDE)
        order = wide * count_c
        f32 = jnp.float32
        return pl.pallas_call(
            make_kernel(leaf_n, share, strip),
            out_shape=jax.ShapeDtypeStruct(block.shape, f32),
            in_specs=[pl.BlockSpec(memory_space=pltpu.VMEM)],
            out_specs=pl.BlockSpec(memory_space=pl.ANY),
            scratch_shapes=[
                pltpu.VMEM((wide, wide), f32),
                pltpu.VMEM((wide, 2 * wide), f32),
                pltpu.VMEM((wide, 3 * wide), f32),
                pltpu.VMEM((2, 6, leaf_n, leaf_n), f32),
                pltpu.VMEM((leaf_n, leaf_n), f32),
                pltpu.VMEM((leaf_n, leaf_n), f32),
                pltpu.VMEM((share, order), f32),
                pltpu.VMEM((share, order), f32),
                pltpu.SemaphoreType.DMA((2, SIDE * SIDE)),
                pltpu.SemaphoreType.DMA((12,)),
                pltpu.SemaphoreType.DMA((4, 15)),
                pltpu.SemaphoreType.DMA((4, 15)),
                pltpu.SemaphoreType.DMA((4, 16)),
                pltpu.SemaphoreType.DMA((4, 16)),
                pltpu.SemaphoreType.DMA((2 * SIDE,)),
                pltpu.SemaphoreType.DMA((SIDE, 2)),
            ],
            compiler_params=pltpu.CompilerParams(
                collective_id=0, has_side_effects=True, vmem_limit_bytes=60 * 2**20),
            name="spd_inverse",
        )(block)

    spec = P(("batch", "row"), "col")
    return jax.shard_map(local_fn, mesh=mesh, in_specs=(spec,), out_specs=spec, check_vma=False)
```

```python
import jax
import jax.numpy as jnp
from jax import lax
from jax.experimental import pallas as pl
from jax.experimental.pallas import tpu as pltpu
from jax.sharding import PartitionSpec as P

HIGHEST = lax.Precision.HIGHEST
MESH = pl.DeviceIdType.MESH
SIDE = 4
ROUNDS = 6
ORDER = (
    "A0", "B00", "B01", "C00", "C01", "C03", "B02", "S0", "C02", "C05", "C04", "A1", "S2", "D00",
    "D01", "C06", "C07", "A2", "S1", "D02", "B10", "B11", "C11", "C10", "D03", "B20", "B21", "C20",
    "C21", "C12", "B12", "S3", "C13", "B22", "C14", "C15", "D10", "C23", "C22", "C25", "C24", "C17",
    "D20", "D11", "C16", "C27", "C26", "A5", "D21", "D12", "D13", "B50", "B51", "A3", "P1", "I00",
    "D22", "D23", "C50", "I01", "C51", "P0", "P2", "G100", "B52", "C52", "C53", "C54", "B30", "A4",
    "G101", "C55", "D50", "B31", "C30", "C31", "I10", "I11", "C56", "C57", "D52", "B40", "B41", "G200",
    "D51", "B32", "C32", "C33", "C40", "G201", "C34", "C41", "G210", "D53", "C35", "D30", "B42", "G211",
    "C42", "C43", "C44", "C45", "I20", "C36", "C37", "I21", "D31", "D32", "C47", "D40", "P5", "G320",
    "D33", "C46", "D41", "D42", "G321", "D43", "P3", "G300", "G301", "P4", "G310", "G311", "I30", "I31",
)


def dot_nn(a, b):
    return lax.dot_general(a, b, (((1,), (0,)), ((), ())), precision=HIGHEST, preferred_element_type=jnp.float32)


def dot_nt(a, b):
    return lax.dot_general(a, b, (((1,), (1,)), ((), ())), precision=HIGHEST, preferred_element_type=jnp.float32)


def leaf_inverse(leaf, inv):
    order = leaf.shape[0]
    part = 128
    count = order // part
    rows = lax.broadcasted_iota(jnp.int32, (part, part), 0)
    cols = lax.broadcasted_iota(jnp.int32, (part, part), 1)

    def blk(i, j):
        return leaf[part * i : part * (i + 1), part * j : part * (j + 1)]

    diag = [blk(q, q) for q in range(count)]
    done = [jnp.where(rows == cols, 1.0 / d, 0.0) for d in diag]
    size = 1
    while size < part:
        low = (rows // (2 * size) == cols // (2 * size)) & (rows // size % 2 == 1) & (cols // size % 2 == 0)
        prods = [dot_nn(jnp.where(low, d, 0.0), x) for d, x in zip(diag, done)]
        done = [x - dot_nn(x, t) for x, t in zip(done, prods)]
        size *= 2
    out = {}
    for i in range(count):
        out[i, i] = done[i]
    for gap in range(1, count):
        for j in range(count - gap):
            i = j + gap
            acc = dot_nn(blk(i, j), out[j, j])
            for k in range(j + 1, i):
                acc = acc + dot_nn(blk(i, k), out[k, j])
            out[i, j] = -dot_nn(out[i, i], acc)
    for n, (i, j) in enumerate((i, j) for j in range(count) for i in range(j, count)):
        inv[n] = out[i, j]


def make_kernel(leaf_n, share, strip):
    wide = 2 * leaf_n
    part = leaf_n // 3
    head = 8
    shifts = (0, SIDE - 1, 1, 2)
    DIRS = (1, -1, 1, -1)

    def kernel(own, out, off1, off3, diag, leaf, inv, low, pmat, zmat,
               scat_send, scat_recv, ring_send, ring_recv, pair_send, pair_recv, out_send, out_recv):
        row = lax.axis_index("row")
        y = lax.axis_index("col")
        x = row // 2
        k = row % 2
        me = SIDE * x + y
        def off_part(a, yy):
            if a < 3:
                return off1, (a - 1) + yy
            return off3.at[yy], 0

        def dev(cx, cy, core):
            return {"row": 2 * cx + core, "col": cy}

        barrier = pltpu.get_barrier_semaphore()

        def greet(t, carry):
            @pl.when(t != row * SIDE + y)
            def _():
                pl.semaphore_signal(barrier, inc=1, device_id={"row": t // SIDE, "col": t % SIDE}, device_id_type=MESH)
            return carry

        lax.fori_loop(0, 2 * SIDE * SIDE, greet, 0)
        pl.semaphore_wait(barrier, 2 * SIDE * SIDE - 1)

        def scatter(src_of, dst_of, cond, core, send_row, sem, first=0, last=SIDE * SIDE):
            @pl.when(cond)
            def _():
                def body(m, carry):
                    src, dst = src_of(m), dst_of(m)
                    here = (m == me) & (core == k)

                    @pl.when(here)
                    def _():
                        pltpu.make_async_copy(src, dst, scat_recv.at[sem]).start()

                    @pl.when(jnp.logical_not(here))
                    def _():
                        pltpu.make_async_remote_copy(
                            src_ref=src, dst_ref=dst, send_sem=scat_send.at[send_row], recv_sem=scat_recv.at[sem],
                            device_id=dev(m // SIDE, m % SIDE, core), device_id_type=MESH).start()
                    return carry

                lax.fori_loop(first, last, body, 0)

        PARTS = {0: (0, head), 1: (head, strip - head), 2: (0, strip)}

        def strip_rows(m, core, part):
            start, count = PARTS[part]
            return pl.ds(pl.multiple_of(leaf_n * core + strip * m, 8) + start, count)

        def off_src(part):
            return lambda m: own.at[strip_rows(m, 0, part), :]

        def off_dst(a, yy, part):
            ref, pos = off_part(a, yy)
            return lambda m: ref.at[strip_rows(m, k, part), pl.ds(wide * pos, wide)]

        def off_sem(a, yy, part):
            return {1: 0, 2: 1 + yy, 3: 6 + yy}[a] + (3 if part == 1 else 0)

        def scatter_off(a, part, *span):
            for yy in range(a):
                scatter(off_src(part), off_dst(a, yy, part), (x == a) & (y == yy), k, part % 2, off_sem(a, yy, part),
                        *span)

        def band(m):
            return pl.ds(pl.multiple_of(8 * m, 8), 8)

        def low_at(a):
            return 6 * SIDE + 9 * (a % 2)

        def scatter_low(a):
            core = a // 2
            scatter(lambda m: low.at[:, band(m), :], lambda m: diag.at[core, low_at(a) : low_at(a) + 9, band(m), :],
                    (x == a) & (y == a) & (k == 1), core, 1, 13 + a % 2)

        def scatter_inv(a):
            scatter(lambda m: inv.at[:, band(m), :], lambda m: diag.at[k, 6 * a : 6 * (a + 1), band(m), :],
                    (x == a) & (y == a), k, 0, 9 + a)

        def landed(dst, src_like, sem, is_source):
            @pl.when(is_source)
            def _():
                pltpu.make_async_copy(src_like, dst, scat_recv.at[sem]).wait()

            @pl.when(jnp.logical_not(is_source))
            def _():
                pltpu.make_async_remote_copy(
                    src_ref=src_like, dst_ref=dst, send_sem=scat_send.at[0], recv_sem=scat_recv.at[sem],
                    device_id=dev(x, y, 1 - k), device_id_type=MESH).wait_recv()

        def landed_off(a, places, part):
            for yy in places:
                landed(off_dst(a, yy, part)(me), off_src(part)(me), off_sem(a, yy, part), (x == a) & (y == yy))

        def landed_diag():
            for a in range(SIDE):
                landed(diag.at[k, 6 * a : 6 * (a + 1), band(me), :], inv.at[:, band(me), :], 9 + a, (x == a) & (y == a))
            for q in range(2):
                a = 2 * k + q
                landed(diag.at[k, low_at(q) : low_at(q) + 9, band(me), :], low.at[:, band(me), :], 13 + q,
                       (x == a) & (y == a) & (k == 1))

        def chip_at(core, du, dv):
            cx = (x + du + core * (dv - du)) % SIDE
            cy = (y + dv + core * (du - dv)) % SIDE
            return cx, cy

        def piece(rnd, core, cx, cy):
            m = SIDE * cx + cy
            if rnd == 1:
                return diag.at[core, :, band(m), :]
            if rnd >= 3:
                return off3.at[rnd - 3, strip_rows(m, core, 2), :]
            return off1.at[strip_rows(m, core, rnd // 2), :]

        def strips(rnd, n):
            if rnd == 1:
                return diag.at[0, :, 0 : 8 * n, :]
            if rnd >= 3:
                return off3.at[rnd - 3, 0 : strip * n, :]
            return off1.at[0 : PARTS[rnd // 2][1] * n, :]

        def sent(ref, sem):
            pltpu.make_async_remote_copy(
                src_ref=ref, dst_ref=ref, send_sem=sem, recv_sem=scat_recv.at[0],
                device_id=dev(x, y, 1 - k), device_id_type=MESH).wait_send()

        def ring_copy(rnd, du, dv, tu, tv, idx):
            ref = piece(rnd, k, *chip_at(k, du, dv))
            return pltpu.make_async_remote_copy(
                src_ref=ref, dst_ref=ref, send_sem=ring_send.at[rnd], recv_sem=ring_recv.at[rnd, idx],
                device_id=dev(*chip_at(k, tu, tv), k), device_id_type=MESH)

        def ring_start(*args):
            ring_copy(*args).start()

        def ring_wait(rnd, du, dv, idx):
            ring_copy(rnd, du, dv, 0, 1, idx).wait_recv()

        def pair_start(rnd, g, dv):
            ref = piece(rnd, k, *chip_at(k, shifts[g], dv))
            pltpu.make_async_remote_copy(
                src_ref=ref, dst_ref=ref, send_sem=pair_send.at[rnd], recv_sem=pair_recv.at[rnd],
                device_id=dev(x, y, 1 - k), device_id_type=MESH).start()

        def spread(rnd, g):
            ring_start(rnd, shifts[g], 0, 0, 1, 3 + 3 * g)
            ring_start(rnd, shifts[g], 0, 0, -1, 4 + 3 * g)
            pair_start(rnd, g, 0)

        def stage_a(rnd):
            arrive(rnd)
            ring_start(rnd, 0, 0, 1, 0, 0)
            ring_start(rnd, 0, 0, -1, 0, 1)
            spread(rnd, 0)

        def stage_b(rnd, j):
            ring_wait(rnd, (-1, 1, 2)[j], 0, j)
            if j == 0 and rnd % 2 == 0:
                ring_start(rnd, -1, 0, 1, 0, 2)
            if j == 1 and rnd % 2 == 1:
                ring_start(rnd, 1, 0, -1, 0, 2)
            spread(rnd, j + 1)

        def stage_c(rnd, j):
            g, back = j // 2, j % 2
            from_v = 1 if back else -1
            ring_wait(rnd, shifts[g], from_v, 3 + 3 * g + back)
            if DIRS[g] == -from_v:
                ring_start(rnd, shifts[g], from_v, 0, -from_v, 5 + 3 * g)
            pair_start(rnd, g, from_v)

        def stage_d(rnd, g):
            ring_wait(rnd, shifts[g], 2, 5 + 3 * g)
            pair_start(rnd, g, 2)

        def pair_done(rnd):
            ref = strips(rnd, SIDE * SIDE)
            pltpu.make_async_remote_copy(
                src_ref=ref, dst_ref=ref, send_sem=pair_send.at[rnd], recv_sem=pair_recv.at[rnd],
                device_id=dev(x, y, 1 - k), device_id_type=MESH).wait_recv()

        def column(core, start, count):
            col = diag[core, start : start + count].reshape(part * count, part)
            return col if count == 3 else jnp.concatenate([jnp.zeros((part * (3 - count), part), jnp.float32), col], axis=0)

        def low_of(a):
            return jnp.concatenate([column(a // 2, low_at(a) + 3 * c, 3) for c in range(3)], axis=1)

        def inv_of(i):
            first = 6 * (i // 2)
            return jnp.concatenate([column(i % 2, first + n, c) for n, c in ((0, 3), (3, 2), (5, 1))], axis=1)

        j0 = leaf_n * row + share * y
        rowi = lax.broadcasted_iota(jnp.int32, (share, leaf_n), 0)
        coli = lax.broadcasted_iota(jnp.int32, (share, leaf_n), 1)

        begun = set()

        def subtract(a, kk, h):
            ref, pos = off_part(a, kk)
            lo = wide * a + leaf_n * h
            acc = dot_nt(pmat[:, wide * kk : wide * (kk + 1)],
                         ref[leaf_n * h : leaf_n * (h + 1), wide * pos : wide * (pos + 1)])
            pmat[:, lo : lo + leaf_n] = pmat[:, lo : lo + leaf_n] + acc if (a, h) in begun else acc
            begun.add((a, h))

        def finish(a, h):
            lo = wide * a + leaf_n * h
            rest = jnp.where(rowi + j0 == coli + lo, 1.0, 0.0)
            if a:
                rest = rest - pmat[:, lo : lo + leaf_n]
            if h:
                rest = rest - dot_nt(pmat[:, lo - leaf_n : lo], low_of(a))
            pmat[:, lo : lo + leaf_n] = dot_nt(rest, inv_of(2 * a + h))

        def out_copy(i, yy, src_y):
            return pltpu.make_async_remote_copy(
                src_ref=zmat.at[:, leaf_n * i : leaf_n * (i + 1)],
                dst_ref=out.at[pl.ds(pl.multiple_of(share * src_y, 8), share), leaf_n * (i % 2) : leaf_n * (i % 2 + 1)],
                send_sem=out_send.at[i], recv_sem=out_recv.at[src_y, i % 2],
                device_id={"row": row, "col": yy}, device_id_type=MESH)

        def out_local(i):
            return pltpu.make_async_copy(
                zmat.at[:, leaf_n * i : leaf_n * (i + 1)],
                out.at[pl.ds(pl.multiple_of(share * y, 8), share), leaf_n * (i % 2) : leaf_n * (i % 2 + 1)],
                out_send.at[i])

        def ship(i, wait):
            @pl.when(y == i // 2)
            def _():
                c = out_local(i)
                c.wait() if wait else c.start()

            @pl.when(y != i // 2)
            def _():
                c = out_copy(i, i // 2, y)
                c.wait_send() if wait else c.start()

        def backward(a):
            lo, hi = wide * a, wide * a + leaf_n

            def rest(start, skip):
                r = pmat[:, start : start + leaf_n]
                for b in range(a + 1, SIDE):
                    ref, pos = off_part(b, a)
                    first = wide * pos + skip
                    r = r - dot_nn(zmat[:, wide * b : wide * (b + 1)], ref[:, first : first + leaf_n])
                return r

            z1 = dot_nn(rest(hi, leaf_n), inv_of(2 * a + 1))
            zmat[:, hi : hi + leaf_n] = z1
            ship(2 * a + 1, False)
            zmat[:, lo:hi] = dot_nn(rest(lo, 0) - dot_nn(z1, low_of(a)), inv_of(2 * a))
            ship(2 * a, False)

        with jax.named_scope("scatter_send"):
            for p in range(2):
                for a in (1, 2):
                    scatter_off(a, p)

            @pl.when((x == y) & (k == 1))
            def _():
                for c in range(3):
                    for r in range(3):
                        low[3 * c + r] = own[part * r : part * (r + 1), part * c : part * (c + 1)]

            for a in range(SIDE):
                scatter_low(a)

        with jax.named_scope("leaf"):
            @pl.when((x == y) & (k == 0))
            def _():
                leaf[...] = own[:, :leaf_n]

            @pl.when((x == y) & (k == 1))
            def _():
                leaf[...] = own[:, leaf_n:]

            @pl.when(x == y)
            def _():
                leaf_inverse(leaf, inv)

            for a in range(SIDE):
                scatter_inv(a)

        def step(name, fn, *args):
            with jax.named_scope(name):
                fn(*args)

        def arrive(rnd):
            if rnd == 1:
                landed_diag()
            elif rnd < 3:
                landed_off(1, (0,), rnd // 2)
                landed_off(2, (0, 1), rnd // 2)
            else:
                landed_off(3, (rnd - 3,), 2)

        stages = {"A": stage_a, "B": stage_b, "C": stage_c, "D": stage_d, "P": pair_done, "G": subtract, "I": finish,
                  "S": lambda q: scatter_off(3, 2, SIDE * q, SIDE * (q + 1))}
        for token in ORDER:
            step(token, stages[token[0]], *(int(d) for d in token[1:]))
        for a in range(SIDE - 1, -1, -1):
            step(f"backward{a}", backward, a)

        for rnd in range(ROUNDS):
            sent(strips(rnd, SIDE * SIDE - 1), ring_send.at[rnd])
            sent(strips(rnd, SIDE * SIDE), pair_send.at[rnd])
        others = SIDE * SIDE - 1
        for p in range(2):
            @pl.when((y < x) & (x < 3))
            def _():
                sent(off1.at[0 : PARTS[p][1] * others, 0:wide], scat_send.at[p])

        @pl.when((y < x) & (x == 3))
        def _():
            sent(off1.at[0 : strip * others, 0:wide], scat_send.at[0])

        @pl.when(x == y)
        def _():
            sent(inv.at[:, 0 : 8 * others, :], scat_send.at[0])

        for core in range(2):
            @pl.when((x == y) & (k == 1) & (x // 2 == core))
            def _():
                sent(low.at[:, 0 : 8 * (others + 1 - core), :], scat_send.at[1])
        for i in range(2 * SIDE):
            ship(i, True)
        for yy in range(SIDE):
            @pl.when(y != yy)
            def _():
                for h in range(2):
                    out_copy(h, y, yy).wait_recv()

    return kernel


def solution(mesh):
    count_c = mesh.shape["col"]

    def local_fn(block):
        leaf_n, wide = block.shape
        share = leaf_n // count_c
        strip = leaf_n // (SIDE * SIDE)
        order = wide * count_c
        f32 = jnp.float32
        return pl.pallas_call(
            make_kernel(leaf_n, share, strip),
            out_shape=jax.ShapeDtypeStruct(block.shape, f32),
            in_specs=[pl.BlockSpec(memory_space=pltpu.VMEM)],
            out_specs=pl.BlockSpec(memory_space=pl.ANY),
            scratch_shapes=[
                pltpu.VMEM((wide, 3 * wide), f32),
                pltpu.VMEM((3, wide, wide), f32),
                pltpu.VMEM((2, 42, leaf_n // 3, leaf_n // 3), f32),
                pltpu.VMEM((leaf_n, leaf_n), f32),
                pltpu.VMEM((6, leaf_n // 3, leaf_n // 3), f32),
                pltpu.VMEM((9, leaf_n // 3, leaf_n // 3), f32),
                pltpu.VMEM((share, order), f32),
                pltpu.VMEM((share, order), f32),
                pltpu.SemaphoreType.DMA((2,)),
                pltpu.SemaphoreType.DMA((15,)),
                pltpu.SemaphoreType.DMA((ROUNDS,)),
                pltpu.SemaphoreType.DMA((ROUNDS, 15)),
                pltpu.SemaphoreType.DMA((ROUNDS,)),
                pltpu.SemaphoreType.DMA((ROUNDS,)),
                pltpu.SemaphoreType.DMA((2 * SIDE,)),
                pltpu.SemaphoreType.DMA((SIDE, 2)),
            ],
            compiler_params=pltpu.CompilerParams(
                collective_id=0, has_side_effects=True, vmem_limit_bytes=60 * 2**20),
            name="spd_inverse",
        )(block)

    spec = P(("batch", "row"), "col")
    return jax.shard_map(local_fn, mesh=mesh, in_specs=(spec,), out_specs=spec, check_vma=False)
```

```python
import jax
import jax.numpy as jnp
from jax import lax
from jax.experimental import pallas as pl
from jax.experimental.pallas import tpu as pltpu
from jax.sharding import PartitionSpec as P

HIGHEST = lax.Precision.HIGHEST
MESH = pl.DeviceIdType.MESH
SIDE = 4
ROUNDS = 6
ALONG_X = ()
ORDER = (
    "A0", "B00", "T0", "B01", "C00", "C01", "A1", "T1", "C03", "B02", "C02", "C05", "C04", "S0",
    "A2", "D00", "B10", "B11", "C11", "D01", "S1", "C10", "C07", "B20", "C06", "B21", "S2", "D02",
    "C20", "C21", "B12", "B22", "C13", "S3", "C12", "C15", "C14", "D03", "C23", "D10", "C25", "C22",
    "C24", "A4", "C17", "D20", "C27", "B40", "B41", "C16", "D11", "D21", "C26", "C41", "B42", "A3",
    "D12", "D13", "P1", "I00", "B30", "B31", "I01", "D22", "D23", "C40", "C43", "C42", "A5", "C45",
    "P0", "P2", "G100", "B32", "C44", "C46", "C47", "G101", "C30", "I10", "B50", "B51", "C31", "I11",
    "C32", "C33", "C34", "C35", "G200", "D40", "D41", "C50", "G201", "B52", "C51", "C36", "G210", "C37",
    "D30", "D42", "D43", "G211", "C52", "C53", "I20", "C54", "C55", "I21", "D50", "D31", "C57", "D32",
    "P4", "G310", "C56", "D33", "G311", "D51", "D52", "D53", "P3", "G300", "G301", "P5", "G320", "G321",
    "I30", "I31",
)


def dot_nn(a, b):
    return lax.dot_general(a, b, (((1,), (0,)), ((), ())), precision=HIGHEST, preferred_element_type=jnp.float32)


def dot_nt(a, b):
    return lax.dot_general(a, b, (((1,), (1,)), ((), ())), precision=HIGHEST, preferred_element_type=jnp.float32)


def leaf_inverse(leaf, inv):
    order = leaf.shape[0]
    part = 128
    count = order // part
    rows = lax.broadcasted_iota(jnp.int32, (part, part), 0)
    cols = lax.broadcasted_iota(jnp.int32, (part, part), 1)

    def blk(i, j):
        return leaf[part * i : part * (i + 1), part * j : part * (j + 1)]

    diag = [blk(q, q) for q in range(count)]
    done = [jnp.where(rows == cols, 1.0 / d, 0.0) for d in diag]

    def merge(level, xs):
        rbit, cbit = rows >> level, cols >> level
        low = (rbit == cbit + 1) & (cbit & 1 == 0)
        prods = [dot_nn(jnp.where(low, blk(q, q), 0.0), x) for q, x in enumerate(xs)]
        return tuple(x - dot_nn(x, t) for x, t in zip(xs, prods))

    done = lax.fori_loop(0, part.bit_length() - 1, merge, tuple(done))
    out = {}
    for i in range(count):
        out[i, i] = done[i]
    for gap in range(1, count):
        for j in range(count - gap):
            i = j + gap
            acc = dot_nn(blk(i, j), out[j, j])
            for k in range(j + 1, i):
                acc = acc + dot_nn(blk(i, k), out[k, j])
            out[i, j] = -dot_nn(out[i, i], acc)
    for n, (i, j) in enumerate((i, j) for j in range(count) for i in range(j, count)):
        inv[n] = out[i, j]


def make_kernel(leaf_n, share, strip):
    wide = 2 * leaf_n
    part = leaf_n // 3
    head = 8
    shifts = (0, SIDE - 1, 1, 2)
    DIRS = (1, -1, 1, -1)

    def kernel(own, out, off, diag, leaf, inv, low, pmat, zmat,
               scat_send, scat_recv, ring_send, ring_recv, pair_send, pair_recv, out_send, out_recv):
        row = lax.axis_index("row")
        y = lax.axis_index("col")
        x = row // 2
        k = row % 2
        me = SIDE * x + y
        def off_of(a, yy):
            return off.at[a * (a - 1) // 2 + yy]

        def dev(cx, cy, core):
            return {"row": 2 * cx + core, "col": cy}

        barrier = pltpu.get_barrier_semaphore()

        def greet(t, carry):
            @pl.when(t != row * SIDE + y)
            def _():
                pl.semaphore_signal(barrier, inc=1, device_id={"row": t // SIDE, "col": t % SIDE}, device_id_type=MESH)
            return carry

        lax.fori_loop(0, 2 * SIDE * SIDE, greet, 0)
        pl.semaphore_wait(barrier, 2 * SIDE * SIDE - 1)

        def scatter(src_of, dst_of, cond, core, send_row, sem, first=0, last=SIDE * SIDE):
            @pl.when(cond)
            def _():
                def body(m, carry):
                    src, dst = src_of(m), dst_of(m)
                    here = (m == me) & (core == k)

                    @pl.when(here)
                    def _():
                        pltpu.make_async_copy(src, dst, scat_recv.at[sem]).start()

                    @pl.when(jnp.logical_not(here))
                    def _():
                        pltpu.make_async_remote_copy(
                            src_ref=src, dst_ref=dst, send_sem=scat_send.at[send_row], recv_sem=scat_recv.at[sem],
                            device_id=dev(m // SIDE, m % SIDE, core), device_id_type=MESH).start()
                    return carry

                lax.fori_loop(first, last, body, 0)

        PARTS = {0: (0, head), 1: (head, strip - head), 2: (0, strip)}

        def strip_rows(m, core, part):
            start, count = PARTS[part]
            return pl.ds(pl.multiple_of(leaf_n * core + strip * m, 8) + start, count)

        def off_src(part):
            return lambda m: own.at[strip_rows(m, 0, part), :]

        def off_dst(a, yy, part):
            return lambda m: off_of(a, yy).at[strip_rows(m, k, part), :]

        def off_sem(a, yy, part):
            return {1: 0, 2: 1 + yy, 3: 6 + yy}[a] + (3 if part == 1 else 0)

        def scatter_off(a, part, *span):
            for yy in range(a):
                scatter(off_src(part), off_dst(a, yy, part), (x == a) & (y == yy), k, part % 2, off_sem(a, yy, part),
                        *span)

        def band(m):
            return pl.ds(pl.multiple_of(8 * m, 8), 8)

        def low_at(a):
            return 6 * SIDE + 9 * (a % 2)

        def scatter_low(a):
            core = a // 2
            scatter(lambda m: low.at[:, band(m), :], lambda m: diag.at[core, low_at(a) : low_at(a) + 9, band(m), :],
                    (x == a) & (y == a) & (k == 1), core, 1, 13 + a % 2)

        def scatter_inv(a):
            scatter(lambda m: inv.at[:, band(m), :], lambda m: diag.at[k, 6 * a : 6 * (a + 1), band(m), :],
                    (x == a) & (y == a), k, 0, 9 + a)

        def landed(dst, src_like, sem, is_source):
            @pl.when(is_source)
            def _():
                pltpu.make_async_copy(src_like, dst, scat_recv.at[sem]).wait()

            @pl.when(jnp.logical_not(is_source))
            def _():
                pltpu.make_async_remote_copy(
                    src_ref=src_like, dst_ref=dst, send_sem=scat_send.at[0], recv_sem=scat_recv.at[sem],
                    device_id=dev(x, y, 1 - k), device_id_type=MESH).wait_recv()

        def landed_off(a, places, part):
            for yy in places:
                landed(off_dst(a, yy, part)(me), off_src(part)(me), off_sem(a, yy, part), (x == a) & (y == yy))

        def landed_diag():
            for a in range(SIDE):
                landed(diag.at[k, 6 * a : 6 * (a + 1), band(me), :], inv.at[:, band(me), :], 9 + a, (x == a) & (y == a))
            for q in range(2):
                a = 2 * k + q
                landed(diag.at[k, low_at(q) : low_at(q) + 9, band(me), :], low.at[:, band(me), :], 13 + q,
                       (x == a) & (y == a) & (k == 1))

        def chip_at(rnd, du, dv):
            turn = 0 if rnd in ALONG_X else k
            cx = (x + du + turn * (dv - du)) % SIDE
            cy = (y + dv + turn * (du - dv)) % SIDE
            return cx, cy

        def piece(rnd, core, cx, cy):
            m = SIDE * cx + cy
            if rnd == 1:
                return diag.at[core, :, band(m), :]
            if rnd >= 3:
                return off.at[rnd, strip_rows(m, core, 2), :]
            return off.at[0:3, strip_rows(m, core, rnd // 2), :]

        def strips(rnd, n):
            if rnd == 1:
                return diag.at[0, :, 0 : 8 * n, :]
            if rnd >= 3:
                return off.at[rnd, 0 : strip * n, :]
            return off.at[0:3, 0 : PARTS[rnd // 2][1] * n, :]

        def sent(ref, sem):
            pltpu.make_async_remote_copy(
                src_ref=ref, dst_ref=ref, send_sem=sem, recv_sem=scat_recv.at[0],
                device_id=dev(x, y, 1 - k), device_id_type=MESH).wait_send()

        def ring_copy(rnd, du, dv, tu, tv, idx):
            ref = piece(rnd, k, *chip_at(rnd, du, dv))
            return pltpu.make_async_remote_copy(
                src_ref=ref, dst_ref=ref, send_sem=ring_send.at[rnd], recv_sem=ring_recv.at[rnd, idx],
                device_id=dev(*chip_at(rnd, tu, tv), k), device_id_type=MESH)

        def ring_start(*args):
            ring_copy(*args).start()

        def ring_wait(rnd, du, dv, idx):
            ring_copy(rnd, du, dv, 0, 1, idx).wait_recv()

        def pair_start(rnd, g, dv):
            ref = piece(rnd, k, *chip_at(rnd, shifts[g], dv))
            pltpu.make_async_remote_copy(
                src_ref=ref, dst_ref=ref, send_sem=pair_send.at[rnd], recv_sem=pair_recv.at[rnd],
                device_id=dev(x, y, 1 - k), device_id_type=MESH).start()

        def spread(rnd, g):
            ring_start(rnd, shifts[g], 0, 0, 1, 3 + 3 * g)
            ring_start(rnd, shifts[g], 0, 0, -1, 4 + 3 * g)
            pair_start(rnd, g, 0)

        def stage_a(rnd):
            arrive(rnd)
            ring_start(rnd, 0, 0, 1, 0, 0)
            ring_start(rnd, 0, 0, -1, 0, 1)
            spread(rnd, 0)

        def stage_b(rnd, j):
            ring_wait(rnd, (-1, 1, 2)[j], 0, j)
            if j == 0 and rnd % 2 == 0:
                ring_start(rnd, -1, 0, 1, 0, 2)
            if j == 1 and rnd % 2 == 1:
                ring_start(rnd, 1, 0, -1, 0, 2)
            spread(rnd, j + 1)

        def stage_c(rnd, j):
            g, back = j // 2, j % 2
            from_v = 1 if back else -1
            ring_wait(rnd, shifts[g], from_v, 3 + 3 * g + back)
            if DIRS[g] == -from_v:
                ring_start(rnd, shifts[g], from_v, 0, -from_v, 5 + 3 * g)
            pair_start(rnd, g, from_v)

        def stage_d(rnd, g):
            ring_wait(rnd, shifts[g], 2, 5 + 3 * g)
            pair_start(rnd, g, 2)

        def pair_done(rnd):
            ref = strips(rnd, SIDE * SIDE)
            pltpu.make_async_remote_copy(
                src_ref=ref, dst_ref=ref, send_sem=pair_send.at[rnd], recv_sem=pair_recv.at[rnd],
                device_id=dev(x, y, 1 - k), device_id_type=MESH).wait_recv()

        def column(core, start, count):
            col = diag[core, pl.ds(start, count)].reshape(part * count, part)
            return col if count == 3 else jnp.concatenate([jnp.zeros((part * (3 - count), part), jnp.float32), col], axis=0)

        def low_of(a):
            return jnp.concatenate([column(a // 2, low_at(a) + 3 * c, 3) for c in range(3)], axis=1)

        def inv_of(a, h):
            return jnp.concatenate([column(h, 6 * a + n, c) for n, c in ((0, 3), (3, 2), (5, 1))], axis=1)

        j0 = leaf_n * row + share * y
        rowi = lax.broadcasted_iota(jnp.int32, (share, leaf_n), 0)
        coli = lax.broadcasted_iota(jnp.int32, (share, leaf_n), 1)

        begun = set()

        def subtract(a, kk, h):
            lo = wide * a + leaf_n * h
            acc = dot_nt(pmat[:, wide * kk : wide * (kk + 1)], off_of(a, kk)[leaf_n * h : leaf_n * (h + 1), :])
            pmat[:, lo : lo + leaf_n] = pmat[:, lo : lo + leaf_n] + acc if (a, h) in begun else acc
            begun.add((a, h))

        def finish(a, h):
            lo = wide * a + leaf_n * h
            rest = jnp.where(rowi + j0 == coli + lo, 1.0, 0.0)
            if a:
                rest = rest - pmat[:, lo : lo + leaf_n]
            if h:
                rest = rest - dot_nt(pmat[:, lo - leaf_n : lo], low_of(a))
            pmat[:, lo : lo + leaf_n] = dot_nt(rest, inv_of(a, h))

        def leaf_cols(i):
            return pl.ds(pl.multiple_of(leaf_n * i, 128), leaf_n)

        def out_at(src_y, h):
            return out.at[pl.ds(pl.multiple_of(share * src_y, 8), share), leaf_cols(h)]

        def out_copy(a, h, src_y, yy):
            return pltpu.make_async_remote_copy(
                src_ref=zmat.at[:, leaf_cols(2 * a + h)], dst_ref=out_at(src_y, h),
                send_sem=out_send.at[2 * a + h], recv_sem=out_recv.at[src_y, h],
                device_id={"row": row, "col": yy}, device_id_type=MESH)

        def ship(a, h, wait):
            @pl.when(y == a)
            def _():
                c = pltpu.make_async_copy(zmat.at[:, leaf_cols(2 * a + h)], out_at(y, h), out_send.at[2 * a + h])
                c.wait() if wait else c.start()

            @pl.when(y != a)
            def _():
                c = out_copy(a, h, y, a)
                c.wait_send() if wait else c.start()

        def backward(a):
            def rest(h):
                r = pmat[:, leaf_cols(2 * a + h)]
                for b in range(a + 1, SIDE):
                    blk = off_of(b, a)[:, leaf_n * h : leaf_n * (h + 1)]
                    r = r - dot_nn(zmat[:, wide * b : wide * (b + 1)], blk)
                return r

            z1 = dot_nn(rest(1), inv_of(a, 1))
            zmat[:, leaf_cols(2 * a + 1)] = z1
            ship(a, 1, False)
            zmat[:, leaf_cols(2 * a)] = dot_nn(rest(0) - dot_nn(z1, low_of(a)), inv_of(a, 0))
            ship(a, 0, False)

        with jax.named_scope("scatter_send"):
            for a in (1, 2):
                scatter_off(a, 0)

            @pl.when((x == y) & (k == 1))
            def _():
                for c in range(3):
                    for r in range(3):
                        low[3 * c + r] = own[part * r : part * (r + 1), part * c : part * (c + 1)]

            for a in range(SIDE):
                scatter_low(a)

        with jax.named_scope("leaf"):
            @pl.when((x == y) & (k == 0))
            def _():
                leaf[...] = own[:, :leaf_n]

            @pl.when((x == y) & (k == 1))
            def _():
                leaf[...] = own[:, leaf_n:]

            @pl.when(x == y)
            def _():
                leaf_inverse(leaf, inv)

            for a in range(SIDE):
                scatter_inv(a)

        def step(name, fn, *args):
            with jax.named_scope(name):
                fn(*args)

        def arrive(rnd):
            if rnd == 1:
                landed_diag()
            elif rnd < 3:
                landed_off(1, (0,), rnd // 2)
                landed_off(2, (0, 1), rnd // 2)
            else:
                landed_off(3, (rnd - 3,), 2)

        def scatter_rest(q):
            for a in (1, 2):
                scatter_off(a, 1, 8 * q, 8 * (q + 1))

        stages = {"A": stage_a, "B": stage_b, "C": stage_c, "D": stage_d, "P": pair_done, "G": subtract, "I": finish,
                  "S": lambda q: scatter_off(3, 2, SIDE * q, SIDE * (q + 1)), "T": scatter_rest}
        for token in ORDER:
            step(token, stages[token[0]], *(int(d) for d in token[1:]))
        for a in range(SIDE - 1, -1, -1):
            step(f"backward{a}", backward, a)

        for rnd in range(ROUNDS):
            sent(strips(rnd, SIDE * SIDE - 1), ring_send.at[rnd])
            sent(strips(rnd, SIDE * SIDE), pair_send.at[rnd])
        others = SIDE * SIDE - 1
        for p in range(2):
            @pl.when((y < x) & (x < 3))
            def _():
                sent(off.at[0, 0 : PARTS[p][1] * others, :], scat_send.at[p])

        @pl.when((y < x) & (x == 3))
        def _():
            sent(off.at[0, 0 : strip * others, :], scat_send.at[0])

        @pl.when(x == y)
        def _():
            sent(inv.at[:, 0 : 8 * others, :], scat_send.at[0])

        for core in range(2):
            @pl.when((x == y) & (k == 1) & (x // 2 == core))
            def _():
                sent(low.at[:, 0 : 8 * (others + 1 - core), :], scat_send.at[1])
        for a in range(SIDE):
            for h in range(2):
                ship(a, h, True)
        for yy in range(SIDE):
            @pl.when(y != yy)
            def _():
                for h in range(2):
                    out_copy(0, h, yy, y).wait_recv()

    return kernel


def solution(mesh):
    count_c = mesh.shape["col"]

    def local_fn(block):
        leaf_n, wide = block.shape
        share = leaf_n // count_c
        strip = leaf_n // (SIDE * SIDE)
        order = wide * count_c
        f32 = jnp.float32
        return pl.pallas_call(
            make_kernel(leaf_n, share, strip),
            out_shape=jax.ShapeDtypeStruct(block.shape, f32),
            in_specs=[pl.BlockSpec(memory_space=pltpu.VMEM)],
            out_specs=pl.BlockSpec(memory_space=pl.ANY),
            scratch_shapes=[
                pltpu.VMEM((6, wide, wide), f32),
                pltpu.VMEM((2, 42, leaf_n // 3, leaf_n // 3), f32),
                pltpu.VMEM((leaf_n, leaf_n), f32),
                pltpu.VMEM((6, leaf_n // 3, leaf_n // 3), f32),
                pltpu.VMEM((9, leaf_n // 3, leaf_n // 3), f32),
                pltpu.VMEM((share, order), f32),
                pltpu.VMEM((share, order), f32),
                pltpu.SemaphoreType.DMA((2,)),
                pltpu.SemaphoreType.DMA((15,)),
                pltpu.SemaphoreType.DMA((ROUNDS,)),
                pltpu.SemaphoreType.DMA((ROUNDS, 15)),
                pltpu.SemaphoreType.DMA((ROUNDS,)),
                pltpu.SemaphoreType.DMA((ROUNDS,)),
                pltpu.SemaphoreType.DMA((2 * SIDE,)),
                pltpu.SemaphoreType.DMA((SIDE, 2)),
            ],
            compiler_params=pltpu.CompilerParams(
                collective_id=0, has_side_effects=True, vmem_limit_bytes=60 * 2**20),
            name="spd_inverse",
        )(block)

    spec = P(("batch", "row"), "col")
    return jax.shard_map(local_fn, mesh=mesh, in_specs=(spec,), out_specs=spec, check_vma=False)
```

```python
import jax
import jax.numpy as jnp
from jax import lax
from jax.experimental import pallas as pl
from jax.experimental.pallas import tpu as pltpu
from jax.sharding import PartitionSpec as P

HIGHEST = lax.Precision.HIGHEST
MESH = pl.DeviceIdType.MESH
SIDE = 4
ROUNDS = 6
ORDER = (
    "A0", "T0", "B00", "B01", "T1", "C00", "C01", "A1", "C03", "A2", "B02", "C02", "C05", "C04",
    "D00", "S0", "B10", "B11", "C11", "D01", "C10", "B20", "S1", "B21", "C20", "C21", "C06", "D02",
    "C07", "S2", "B12", "C13", "B22", "C12", "C15", "C14", "C23", "S3", "D10", "C25", "D03", "C22",
    "C17", "C24", "D20", "D11", "C27", "C16", "A4", "A5", "D21", "C26", "D13", "D12", "B40", "B41",
    "P1", "I00", "B50", "B51", "I01", "D22", "D23", "C41", "C40", "C51", "A3", "B42", "C43", "C50",
    "P0", "P2", "G100", "C42", "C45", "G101", "B52", "C44", "C53", "I10", "B30", "B31", "C52", "I11",
    "C31", "C54", "C55", "D40", "G200", "C30", "C47", "D41", "C46", "G201", "B32", "D50", "G210", "C56",
    "C57", "D42", "D51", "G211", "C32", "C33", "C34", "C35", "I20", "D43", "D52", "I21", "C37", "D30",
    "D53", "P4", "G310", "C36", "D31", "D32", "G311", "P5", "D33", "H32", "P3", "H30", "I30", "I31",
)


def dot_nn(a, b):
    return lax.dot_general(a, b, (((1,), (0,)), ((), ())), precision=HIGHEST, preferred_element_type=jnp.float32)


def dot_nt(a, b):
    return lax.dot_general(a, b, (((1,), (1,)), ((), ())), precision=HIGHEST, preferred_element_type=jnp.float32)


def leaf_inverse(leaf, inv):
    order = leaf.shape[0]
    part = 128
    count = order // part
    rows = lax.broadcasted_iota(jnp.int32, (part, part), 0)
    cols = lax.broadcasted_iota(jnp.int32, (part, part), 1)

    def blk(i, j):
        return leaf[part * i : part * (i + 1), part * j : part * (j + 1)]

    diag = [blk(q, q) for q in range(count)]
    done = [jnp.where(rows == cols, 1.0 / d, 0.0) for d in diag]

    def merge(level, xs):
        rbit, cbit = rows >> level, cols >> level
        low = (rbit == cbit + 1) & (cbit & 1 == 0)
        prods = [dot_nn(jnp.where(low, blk(q, q), 0.0), x) for q, x in enumerate(xs)]
        return tuple(x - dot_nn(x, t) for x, t in zip(xs, prods))

    done = lax.fori_loop(0, part.bit_length() - 1, merge, tuple(done))
    out = {}
    for i in range(count):
        out[i, i] = done[i]
    for gap in range(1, count):
        for j in range(count - gap):
            i = j + gap
            acc = dot_nn(blk(i, j), out[j, j])
            for k in range(j + 1, i):
                acc = acc + dot_nn(blk(i, k), out[k, j])
            out[i, j] = -dot_nn(out[i, i], acc)
    for n, (i, j) in enumerate((i, j) for j in range(count) for i in range(j, count)):
        inv[n] = out[i, j]


def make_kernel(leaf_n, share, strip):
    wide = 2 * leaf_n
    part = leaf_n // 3
    head = 8
    shifts = (0, SIDE - 1, 1, 2)
    DIRS = (1, -1, 1, -1)

    def kernel(own, out, off, diag, leaf, inv, low, pmat, zmat,
               scat_send, scat_recv, ring_send, ring_recv, pair_send, pair_recv, out_send, out_recv):
        row = lax.axis_index("row")
        y = lax.axis_index("col")
        x = row // 2
        k = row % 2
        me = SIDE * x + y
        def off_of(a, yy):
            return off.at[a * (a - 1) // 2 + yy]

        def dev(cx, cy, core):
            return {"row": 2 * cx + core, "col": cy}

        barrier = pltpu.get_barrier_semaphore()

        def greet(t, carry):
            @pl.when(t != row * SIDE + y)
            def _():
                pl.semaphore_signal(barrier, inc=1, device_id={"row": t // SIDE, "col": t % SIDE}, device_id_type=MESH)
            return carry

        lax.fori_loop(0, 2 * SIDE * SIDE, greet, 0)
        pl.semaphore_wait(barrier, 2 * SIDE * SIDE - 1)

        def scatter(src_of, dst_of, cond, core, send_row, sem, first=0, last=SIDE * SIDE):
            @pl.when(cond)
            def _():
                def body(m, carry):
                    src, dst = src_of(m), dst_of(m)
                    here = (m == me) & (core == k)

                    @pl.when(here)
                    def _():
                        pltpu.make_async_copy(src, dst, scat_recv.at[sem]).start()

                    @pl.when(jnp.logical_not(here))
                    def _():
                        pltpu.make_async_remote_copy(
                            src_ref=src, dst_ref=dst, send_sem=scat_send.at[send_row], recv_sem=scat_recv.at[sem],
                            device_id=dev(m // SIDE, m % SIDE, core), device_id_type=MESH).start()
                    return carry

                lax.fori_loop(first, last, body, 0)

        PARTS = {0: (0, head), 1: (head, strip - head), 2: (0, strip)}

        def strip_rows(m, core, part):
            start, count = PARTS[part]
            return pl.ds(pl.multiple_of(leaf_n * core + strip * m, 8) + start, count)

        def off_src(part):
            return lambda m: own.at[strip_rows(m, 0, part), :]

        def off_dst(a, yy, part):
            return lambda m: off_of(a, yy).at[strip_rows(m, k, part), :]

        def off_sem(a, yy, part):
            return {1: 0, 2: 1 + yy, 3: 6 + yy}[a] + (3 if part == 1 else 0)

        def scatter_off(a, part, *span):
            for yy in range(a):
                scatter(off_src(part), off_dst(a, yy, part), (x == a) & (y == yy), k, part % 2, off_sem(a, yy, part),
                        *span)

        def band(m):
            return pl.ds(pl.multiple_of(8 * m, 8), 8)

        def low_at(a):
            return 6 * SIDE + 9 * (a % 2)

        def scatter_low(a):
            core = a // 2
            scatter(lambda m: low.at[:, band(m), :], lambda m: diag.at[core, low_at(a) : low_at(a) + 9, band(m), :],
                    (x == a) & (y == a) & (k == 1), core, 1, 13 + a % 2)

        def scatter_inv(a):
            scatter(lambda m: inv.at[:, band(m), :], lambda m: diag.at[k, 6 * a : 6 * (a + 1), band(m), :],
                    (x == a) & (y == a), k, 0, 9 + a)

        def landed(dst, src_like, sem, is_source):
            @pl.when(is_source)
            def _():
                pltpu.make_async_copy(src_like, dst, scat_recv.at[sem]).wait()

            @pl.when(jnp.logical_not(is_source))
            def _():
                pltpu.make_async_remote_copy(
                    src_ref=src_like, dst_ref=dst, send_sem=scat_send.at[0], recv_sem=scat_recv.at[sem],
                    device_id=dev(x, y, 1 - k), device_id_type=MESH).wait_recv()

        def landed_off(a, places, part):
            for yy in places:
                landed(off_dst(a, yy, part)(me), off_src(part)(me), off_sem(a, yy, part), (x == a) & (y == yy))

        def landed_diag():
            for a in range(SIDE):
                landed(diag.at[k, 6 * a : 6 * (a + 1), band(me), :], inv.at[:, band(me), :], 9 + a, (x == a) & (y == a))
            for q in range(2):
                a = 2 * k + q
                landed(diag.at[k, low_at(q) : low_at(q) + 9, band(me), :], low.at[:, band(me), :], 13 + q,
                       (x == a) & (y == a) & (k == 1))

        def relative(du, dv):
            cx = (x + du + k * (dv - du)) % SIDE
            cy = (y + dv + k * (du - dv)) % SIDE
            return cx, cy, SIDE * cx + cy

        chips = {(du, dv): relative(du, dv) for du in range(SIDE) for dv in range(SIDE)}

        def chip_at(du, dv):
            return chips[du % SIDE, dv % SIDE]

        def piece(rnd, core, chip):
            m = chip[2]
            if rnd == 1:
                return diag.at[core, :, band(m), :]
            if rnd >= 3:
                return off.at[rnd, strip_rows(m, core, 2), :]
            return off.at[0:3, strip_rows(m, core, rnd // 2), :]

        def strips(rnd, n):
            if rnd == 1:
                return diag.at[0, :, 0 : 8 * n, :]
            if rnd >= 3:
                return off.at[rnd, 0 : strip * n, :]
            return off.at[0:3, 0 : PARTS[rnd // 2][1] * n, :]

        def sent(ref, sem):
            pltpu.make_async_remote_copy(
                src_ref=ref, dst_ref=ref, send_sem=sem, recv_sem=scat_recv.at[0],
                device_id=dev(x, y, 1 - k), device_id_type=MESH).wait_send()

        def ring_copy(rnd, du, dv, tu, tv, idx):
            ref = piece(rnd, k, chip_at(du, dv))
            return pltpu.make_async_remote_copy(
                src_ref=ref, dst_ref=ref, send_sem=ring_send.at[rnd], recv_sem=ring_recv.at[rnd, idx],
                device_id=dev(*chip_at(tu, tv)[:2], k), device_id_type=MESH)

        def ring_start(*args):
            ring_copy(*args).start()

        def ring_wait(rnd, du, dv, idx):
            ring_copy(rnd, du, dv, 0, 1, idx).wait_recv()

        def pair_start(rnd, g, dv):
            ref = piece(rnd, k, chip_at(shifts[g], dv))
            pltpu.make_async_remote_copy(
                src_ref=ref, dst_ref=ref, send_sem=pair_send.at[rnd], recv_sem=pair_recv.at[rnd],
                device_id=dev(x, y, 1 - k), device_id_type=MESH).start()

        def spread(rnd, g):
            ring_start(rnd, shifts[g], 0, 0, 1, 3 + 3 * g)
            ring_start(rnd, shifts[g], 0, 0, -1, 4 + 3 * g)
            pair_start(rnd, g, 0)

        def stage_a(rnd):
            arrive(rnd)
            ring_start(rnd, 0, 0, 1, 0, 0)
            ring_start(rnd, 0, 0, -1, 0, 1)
            spread(rnd, 0)

        def stage_b(rnd, j):
            ring_wait(rnd, (-1, 1, 2)[j], 0, j)
            if j == 0 and rnd % 2 == 0:
                ring_start(rnd, -1, 0, 1, 0, 2)
            if j == 1 and rnd % 2 == 1:
                ring_start(rnd, 1, 0, -1, 0, 2)
            spread(rnd, j + 1)

        def stage_c(rnd, j):
            g, back = j // 2, j % 2
            from_v = 1 if back else -1
            ring_wait(rnd, shifts[g], from_v, 3 + 3 * g + back)
            if DIRS[g] == -from_v:
                ring_start(rnd, shifts[g], from_v, 0, -from_v, 5 + 3 * g)
            pair_start(rnd, g, from_v)

        def stage_d(rnd, g):
            ring_wait(rnd, shifts[g], 2, 5 + 3 * g)
            pair_start(rnd, g, 2)

        def pair_done(rnd):
            ref = strips(rnd, SIDE * SIDE)
            pltpu.make_async_remote_copy(
                src_ref=ref, dst_ref=ref, send_sem=pair_send.at[rnd], recv_sem=pair_recv.at[rnd],
                device_id=dev(x, y, 1 - k), device_id_type=MESH).wait_recv()

        def column(core, start, count):
            col = diag[core, pl.ds(start, count)].reshape(part * count, part)
            return col if count == 3 else jnp.concatenate([jnp.zeros((part * (3 - count), part), jnp.float32), col], axis=0)

        def low_of(a):
            return jnp.concatenate([column(a // 2, low_at(a) + 3 * c, 3) for c in range(3)], axis=1)

        def inv_of(a, h):
            return jnp.concatenate([column(h, 6 * a + n, c) for n, c in ((0, 3), (3, 2), (5, 1))], axis=1)

        j0 = leaf_n * row + share * y
        rowi = lax.broadcasted_iota(jnp.int32, (share, leaf_n), 0)
        coli = lax.broadcasted_iota(jnp.int32, (share, leaf_n), 1)

        def leaf_cols(i):
            return pl.ds(pl.multiple_of(leaf_n * i, 128), leaf_n)

        begun = set()

        def subtract(a, kk, h):
            place = leaf_cols(2 * a + h)
            rows = pl.ds(pl.multiple_of(leaf_n * h, 8), leaf_n)
            acc = dot_nt(pmat[:, wide * kk : wide * (kk + 1)], off_of(a, kk)[rows, :])
            pmat[:, place] = pmat[:, place] + acc if a in begun else acc

        def subtract_both(a, kk):
            def body(h, carry):
                subtract(a, kk, h)
                return carry

            lax.fori_loop(0, 2, body, 0)
            begun.add(a)

        def subtract_one(a, kk, h):
            subtract(a, kk, h)
            if h:
                begun.add(a)

        def finish(a, h):
            lo = wide * a + leaf_n * h
            rest = jnp.where(rowi + j0 == coli + lo, 1.0, 0.0)
            if a:
                rest = rest - pmat[:, lo : lo + leaf_n]
            if h:
                rest = rest - dot_nt(pmat[:, lo - leaf_n : lo], low_of(a))
            pmat[:, lo : lo + leaf_n] = dot_nt(rest, inv_of(a, h))

        def out_at(src_y, h):
            return out.at[pl.ds(pl.multiple_of(share * src_y, 8), share), leaf_cols(h)]

        def out_copy(a, h, src_y, yy):
            return pltpu.make_async_remote_copy(
                src_ref=zmat.at[:, leaf_cols(2 * a + h)], dst_ref=out_at(src_y, h),
                send_sem=out_send.at[2 * a + h], recv_sem=out_recv.at[src_y, h],
                device_id={"row": row, "col": yy}, device_id_type=MESH)

        def ship(a, h, wait):
            @pl.when(y == a)
            def _():
                c = pltpu.make_async_copy(zmat.at[:, leaf_cols(2 * a + h)], out_at(y, h), out_send.at[2 * a + h])
                c.wait() if wait else c.start()

            @pl.when(y != a)
            def _():
                c = out_copy(a, h, y, a)
                c.wait_send() if wait else c.start()

        def backward(a):
            def rest(h):
                r = pmat[:, leaf_cols(2 * a + h)]
                for b in range(a + 1, SIDE):
                    blk = off_of(b, a)[:, leaf_n * h : leaf_n * (h + 1)]
                    r = r - dot_nn(zmat[:, wide * b : wide * (b + 1)], blk)
                return r

            z1 = dot_nn(rest(1), inv_of(a, 1))
            zmat[:, leaf_cols(2 * a + 1)] = z1
            ship(a, 1, False)
            zmat[:, leaf_cols(2 * a)] = dot_nn(rest(0) - dot_nn(z1, low_of(a)), inv_of(a, 0))
            ship(a, 0, False)

        with jax.named_scope("scatter_send"):
            for a in (1, 2):
                scatter_off(a, 0)

            @pl.when((x == y) & (k == 1))
            def _():
                for c in range(3):
                    for r in range(3):
                        low[3 * c + r] = own[part * r : part * (r + 1), part * c : part * (c + 1)]

            for a in range(SIDE):
                scatter_low(a)

        with jax.named_scope("leaf"):
            @pl.when((x == y) & (k == 0))
            def _():
                leaf[...] = own[:, :leaf_n]

            @pl.when((x == y) & (k == 1))
            def _():
                leaf[...] = own[:, leaf_n:]

            @pl.when(x == y)
            def _():
                leaf_inverse(leaf, inv)

            for a in range(SIDE):
                scatter_inv(a)

        def step(name, fn, *args):
            with jax.named_scope(name):
                fn(*args)

        def arrive(rnd):
            if rnd == 1:
                landed_diag()
            elif rnd < 3:
                landed_off(1, (0,), rnd // 2)
                landed_off(2, (0, 1), rnd // 2)
            else:
                landed_off(3, (rnd - 3,), 2)

        def scatter_rest(q):
            for a in (1, 2):
                scatter_off(a, 1, 8 * q, 8 * (q + 1))

        stages = {"A": stage_a, "B": stage_b, "C": stage_c, "D": stage_d, "P": pair_done, "G": subtract_one, "H": subtract_both, "I": finish,
                  "S": lambda q: scatter_off(3, 2, SIDE * q, SIDE * (q + 1)), "T": scatter_rest}
        for token in ORDER:
            step(token, stages[token[0]], *(int(d) for d in token[1:]))
        for a in range(SIDE - 1, -1, -1):
            step(f"backward{a}", backward, a)

        for rnd in range(ROUNDS):
            sent(strips(rnd, SIDE * SIDE - 1), ring_send.at[rnd])
            sent(strips(rnd, SIDE * SIDE), pair_send.at[rnd])
        others = SIDE * SIDE - 1
        for p in range(2):
            @pl.when((y < x) & (x < 3))
            def _():
                sent(off.at[0, 0 : PARTS[p][1] * others, :], scat_send.at[p])

        @pl.when((y < x) & (x == 3))
        def _():
            sent(off.at[0, 0 : strip * others, :], scat_send.at[0])

        @pl.when(x == y)
        def _():
            sent(inv.at[:, 0 : 8 * others, :], scat_send.at[0])

        for core in range(2):
            @pl.when((x == y) & (k == 1) & (x // 2 == core))
            def _():
                sent(low.at[:, 0 : 8 * (others + 1 - core), :], scat_send.at[1])
        for a in range(SIDE):
            for h in range(2):
                ship(a, h, True)
        for yy in range(SIDE):
            @pl.when(y != yy)
            def _():
                for h in range(2):
                    out_copy(0, h, yy, y).wait_recv()

    return kernel


def solution(mesh):
    count_c = mesh.shape["col"]

    def local_fn(block):
        leaf_n, wide = block.shape
        share = leaf_n // count_c
        strip = leaf_n // (SIDE * SIDE)
        order = wide * count_c
        f32 = jnp.float32
        return pl.pallas_call(
            make_kernel(leaf_n, share, strip),
            out_shape=jax.ShapeDtypeStruct(block.shape, f32),
            in_specs=[pl.BlockSpec(memory_space=pltpu.VMEM)],
            out_specs=pl.BlockSpec(memory_space=pl.ANY),
            scratch_shapes=[
                pltpu.VMEM((6, wide, wide), f32),
                pltpu.VMEM((2, 42, leaf_n // 3, leaf_n // 3), f32),
                pltpu.VMEM((leaf_n, leaf_n), f32),
                pltpu.VMEM((6, leaf_n // 3, leaf_n // 3), f32),
                pltpu.VMEM((9, leaf_n // 3, leaf_n // 3), f32),
                pltpu.VMEM((share, order), f32),
                pltpu.VMEM((share, order), f32),
                pltpu.SemaphoreType.DMA((2,)),
                pltpu.SemaphoreType.DMA((15,)),
                pltpu.SemaphoreType.DMA((ROUNDS,)),
                pltpu.SemaphoreType.DMA((ROUNDS, 15)),
                pltpu.SemaphoreType.DMA((ROUNDS,)),
                pltpu.SemaphoreType.DMA((ROUNDS,)),
                pltpu.SemaphoreType.DMA((2 * SIDE,)),
                pltpu.SemaphoreType.DMA((SIDE, 2)),
            ],
            compiler_params=pltpu.CompilerParams(
                collective_id=0, has_side_effects=True, vmem_limit_bytes=60 * 2**20),
            name="spd_inverse",
        )(block)

    spec = P(("batch", "row"), "col")
    return jax.shard_map(local_fn, mesh=mesh, in_specs=(spec,), out_specs=spec, check_vma=False)
```

```python
import jax
import jax.numpy as jnp
from jax import lax
from jax.experimental import pallas as pl
from jax.experimental.pallas import tpu as pltpu
from jax.sharding import PartitionSpec as P

HIGHEST = lax.Precision.HIGHEST
MESH = pl.DeviceIdType.MESH
SIDE = 4
ROUNDS = 7
ORDER = (
    "A0", "T0", "B00", "B01", "T1", "C00", "C01", "A1", "A2", "C03", "A6", "B02", "C02", "C05",
    "C04", "D00", "B10", "B11", "S0", "C11", "B20", "B21", "C21", "D01", "C10", "B60", "B61", "S1",
    "C20", "C61", "B22", "C60", "C06", "C07", "B12", "S2", "D02", "B62", "C13", "C12", "C15", "C23",
    "C25", "C14", "S3", "C22", "C63", "C24", "C65", "C27", "D10", "D03", "C62", "C64", "C17", "D20",
    "C26", "A4", "C67", "D60", "D11", "D21", "C16", "A5", "D61", "B40", "B41", "C66", "D23", "D12",
    "B50", "B51", "A3", "D13", "D22", "C41", "B42", "P1", "I00", "D63", "D62", "I01", "C51", "C40",
    "P0", "P2", "G100", "B52", "C50", "B30", "C43", "G101", "B31", "C42", "C44", "C45", "I10", "C52",
    "C53", "I11", "C54", "C55", "C31", "C30", "P6", "G200", "C46", "C47", "G201", "C56", "C57", "B32",
    "D40", "G210", "D50", "C32", "C33", "D41", "G211", "D51", "C34", "C35", "I20", "D42", "D43", "I21",
    "D52", "D53", "D30", "C37", "P4", "G310", "C36", "D31", "D32", "G311", "P5", "D33", "H32", "P3",
    "H30", "I30", "I31",
)


def dot_nn(a, b):
    return lax.dot_general(a, b, (((1,), (0,)), ((), ())), precision=HIGHEST, preferred_element_type=jnp.float32)


def dot_nt(a, b):
    return lax.dot_general(a, b, (((1,), (1,)), ((), ())), precision=HIGHEST, preferred_element_type=jnp.float32)


def leaf_inverse(leaf, inv):
    order = leaf.shape[0]
    part = 128
    count = order // part
    rows = lax.broadcasted_iota(jnp.int32, (part, part), 0)
    cols = lax.broadcasted_iota(jnp.int32, (part, part), 1)

    def blk(i, j):
        return leaf[part * i : part * (i + 1), part * j : part * (j + 1)]

    diag = [blk(q, q) for q in range(count)]
    done = [jnp.where(rows == cols, 1.0 / d, 0.0) for d in diag]

    def merge(level, xs):
        rbit, cbit = rows >> level, cols >> level
        low = (rbit == cbit + 1) & (cbit & 1 == 0)
        prods = [dot_nn(jnp.where(low, blk(q, q), 0.0), x) for q, x in enumerate(xs)]
        return tuple(x - dot_nn(x, t) for x, t in zip(xs, prods))

    done = lax.fori_loop(0, part.bit_length() - 1, merge, tuple(done))
    out = {}
    for i in range(count):
        out[i, i] = done[i]
    for gap in range(1, count):
        for j in range(count - gap):
            i = j + gap
            acc = dot_nn(blk(i, j), out[j, j])
            for k in range(j + 1, i):
                acc = acc + dot_nn(blk(i, k), out[k, j])
            out[i, j] = -dot_nn(out[i, i], acc)
    for n, (i, j) in enumerate((i, j) for j in range(count) for i in range(j, count)):
        inv[n] = out[i, j]


def make_kernel(leaf_n, share, strip):
    wide = 2 * leaf_n
    part = leaf_n // 3
    head = 8
    shifts = (0, SIDE - 1, 1, 2)
    DIRS = (1, -1, 1, -1)

    def kernel(own, out, off, diag, leaf, inv, low, pmat, zmat,
               scat_send, scat_recv, ring_send, ring_recv, pair_send, pair_recv, out_send, out_recv):
        row = lax.axis_index("row")
        y = lax.axis_index("col")
        x = row // 2
        k = row % 2
        me = SIDE * x + y
        def off_of(a, yy):
            return off.at[a * (a - 1) // 2 + yy]

        def dev(cx, cy, core):
            return {"row": 2 * cx + core, "col": cy}

        barrier = pltpu.get_barrier_semaphore()

        def greet(t, carry):
            @pl.when(t != row * SIDE + y)
            def _():
                pl.semaphore_signal(barrier, inc=1, device_id={"row": t // SIDE, "col": t % SIDE}, device_id_type=MESH)
            return carry

        lax.fori_loop(0, 2 * SIDE * SIDE, greet, 0)
        pl.semaphore_wait(barrier, 2 * SIDE * SIDE - 1)

        def scatter(src_of, dst_of, cond, core, send_row, sem, first=0, last=SIDE * SIDE):
            @pl.when(cond)
            def _():
                def body(m, carry):
                    src, dst = src_of(m), dst_of(m)
                    here = (m == me) & (core == k)

                    @pl.when(here)
                    def _():
                        pltpu.make_async_copy(src, dst, scat_recv.at[sem]).start()

                    @pl.when(jnp.logical_not(here))
                    def _():
                        pltpu.make_async_remote_copy(
                            src_ref=src, dst_ref=dst, send_sem=scat_send.at[send_row], recv_sem=scat_recv.at[sem],
                            device_id=dev(m // SIDE, m % SIDE, core), device_id_type=MESH).start()
                    return carry

                lax.fori_loop(first, last, body, 0)

        PARTS = {0: (0, head), 1: (head, strip - head), 2: (0, strip)}

        def strip_rows(m, core, part):
            start, count = PARTS[part]
            return pl.ds(pl.multiple_of(leaf_n * core + strip * m, 8) + start, count)

        def off_src(part):
            return lambda m: own.at[strip_rows(m, 0, part), :]

        def off_dst(a, yy, part):
            return lambda m: off_of(a, yy).at[strip_rows(m, k, part), :]

        def off_sem(a, yy, part):
            return {1: 0, 2: 1 + yy, 3: 6 + yy}[a] + (3 if part == 1 else 0)

        def scatter_off(a, part, *span):
            for yy in range(a):
                scatter(off_src(part), off_dst(a, yy, part), (x == a) & (y == yy), k, part % 2, off_sem(a, yy, part),
                        *span)

        def band(m):
            return pl.ds(pl.multiple_of(8 * m, 8), 8)

        def low_at(a):
            return 6 * SIDE + 9 * (a % 2)

        def scatter_low(a):
            core = a // 2
            scatter(lambda m: low.at[:, band(m), :], lambda m: diag.at[core, low_at(a) : low_at(a) + 9, band(m), :],
                    (x == a) & (y == a) & (k == 1), core, 1, 13 + a % 2)

        def scatter_inv(a):
            scatter(lambda m: inv.at[:, band(m), :], lambda m: diag.at[k, 6 * a : 6 * (a + 1), band(m), :],
                    (x == a) & (y == a), k, 0, 9 + a)

        def landed(dst, src_like, sem, is_source):
            @pl.when(is_source)
            def _():
                pltpu.make_async_copy(src_like, dst, scat_recv.at[sem]).wait()

            @pl.when(jnp.logical_not(is_source))
            def _():
                pltpu.make_async_remote_copy(
                    src_ref=src_like, dst_ref=dst, send_sem=scat_send.at[0], recv_sem=scat_recv.at[sem],
                    device_id=dev(x, y, 1 - k), device_id_type=MESH).wait_recv()

        def landed_off(a, places, part):
            for yy in places:
                landed(off_dst(a, yy, part)(me), off_src(part)(me), off_sem(a, yy, part), (x == a) & (y == yy))

        def landed_diag():
            for a in range(SIDE):
                landed(diag.at[k, 6 * a : 6 * (a + 1), band(me), :], inv.at[:, band(me), :], 9 + a, (x == a) & (y == a))
            for q in range(2):
                a = 2 * k + q
                landed(diag.at[k, low_at(q) : low_at(q) + 9, band(me), :], low.at[:, band(me), :], 13 + q,
                       (x == a) & (y == a) & (k == 1))

        def relative(du, dv):
            cx = (x + du + k * (dv - du)) % SIDE
            cy = (y + dv + k * (du - dv)) % SIDE
            return cx, cy, SIDE * cx + cy

        chips = {(du, dv): relative(du, dv) for du in range(SIDE) for dv in range(SIDE)}

        def chip_at(du, dv):
            return chips[du % SIDE, dv % SIDE]

        HEADS = {0: (0, 3, 0), 2: (0, 1, 1), 6: (1, 3, 1)}

        def piece(rnd, core, chip):
            m = chip[2]
            if rnd == 1:
                return diag.at[core, :, band(m), :]
            if rnd in HEADS:
                lo, hi, part = HEADS[rnd]
                return off.at[lo:hi, strip_rows(m, core, part), :]
            return off.at[rnd, strip_rows(m, core, 2), :]

        def strips(rnd, n):
            if rnd == 1:
                return diag.at[0, :, 0 : 8 * n, :]
            if rnd in HEADS:
                lo, hi, part = HEADS[rnd]
                return off.at[lo:hi, 0 : PARTS[part][1] * n, :]
            return off.at[rnd, 0 : strip * n, :]

        def sent(ref, sem):
            pltpu.make_async_remote_copy(
                src_ref=ref, dst_ref=ref, send_sem=sem, recv_sem=scat_recv.at[0],
                device_id=dev(x, y, 1 - k), device_id_type=MESH).wait_send()

        def ring_copy(rnd, du, dv, tu, tv, idx):
            ref = piece(rnd, k, chip_at(du, dv))
            return pltpu.make_async_remote_copy(
                src_ref=ref, dst_ref=ref, send_sem=ring_send.at[rnd], recv_sem=ring_recv.at[rnd, idx],
                device_id=dev(*chip_at(tu, tv)[:2], k), device_id_type=MESH)

        def ring_start(*args):
            ring_copy(*args).start()

        def ring_wait(rnd, du, dv, idx):
            ring_copy(rnd, du, dv, 0, 1, idx).wait_recv()

        def pair_start(rnd, g, dv):
            ref = piece(rnd, k, chip_at(shifts[g], dv))
            pltpu.make_async_remote_copy(
                src_ref=ref, dst_ref=ref, send_sem=pair_send.at[rnd], recv_sem=pair_recv.at[rnd],
                device_id=dev(x, y, 1 - k), device_id_type=MESH).start()

        def spread(rnd, g):
            ring_start(rnd, shifts[g], 0, 0, 1, 3 + 3 * g)
            ring_start(rnd, shifts[g], 0, 0, -1, 4 + 3 * g)
            pair_start(rnd, g, 0)

        def stage_a(rnd):
            arrive(rnd)
            ring_start(rnd, 0, 0, 1, 0, 0)
            ring_start(rnd, 0, 0, -1, 0, 1)
            spread(rnd, 0)

        def stage_b(rnd, j):
            ring_wait(rnd, (-1, 1, 2)[j], 0, j)
            if j == 0 and rnd % 2 == 0:
                ring_start(rnd, -1, 0, 1, 0, 2)
            if j == 1 and rnd % 2 == 1:
                ring_start(rnd, 1, 0, -1, 0, 2)
            spread(rnd, j + 1)

        def stage_c(rnd, j):
            g, back = j // 2, j % 2
            from_v = 1 if back else -1
            ring_wait(rnd, shifts[g], from_v, 3 + 3 * g + back)
            if DIRS[g] == -from_v:
                ring_start(rnd, shifts[g], from_v, 0, -from_v, 5 + 3 * g)
            pair_start(rnd, g, from_v)

        def stage_d(rnd, g):
            ring_wait(rnd, shifts[g], 2, 5 + 3 * g)
            pair_start(rnd, g, 2)

        def pair_done(rnd):
            ref = strips(rnd, SIDE * SIDE)
            pltpu.make_async_remote_copy(
                src_ref=ref, dst_ref=ref, send_sem=pair_send.at[rnd], recv_sem=pair_recv.at[rnd],
                device_id=dev(x, y, 1 - k), device_id_type=MESH).wait_recv()

        def column(core, start, count):
            col = diag[core, pl.ds(start, count)].reshape(part * count, part)
            return col if count == 3 else jnp.concatenate([jnp.zeros((part * (3 - count), part), jnp.float32), col], axis=0)

        def low_of(a):
            return jnp.concatenate([column(a // 2, low_at(a) + 3 * c, 3) for c in range(3)], axis=1)

        def inv_of(a, h):
            return jnp.concatenate([column(h, 6 * a + n, c) for n, c in ((0, 3), (3, 2), (5, 1))], axis=1)

        j0 = leaf_n * row + share * y
        rowi = lax.broadcasted_iota(jnp.int32, (share, leaf_n), 0)
        coli = lax.broadcasted_iota(jnp.int32, (share, leaf_n), 1)

        def leaf_cols(i):
            return pl.ds(pl.multiple_of(leaf_n * i, 128), leaf_n)

        begun = set()

        def subtract(a, kk, h):
            place = leaf_cols(2 * a + h)
            rows = pl.ds(pl.multiple_of(leaf_n * h, 8), leaf_n)
            acc = dot_nt(pmat[:, wide * kk : wide * (kk + 1)], off_of(a, kk)[rows, :])
            pmat[:, place] = pmat[:, place] + acc if a in begun else acc

        def subtract_both(a, kk):
            def body(h, carry):
                subtract(a, kk, h)
                return carry

            lax.fori_loop(0, 2, body, 0)
            begun.add(a)

        def subtract_one(a, kk, h):
            subtract(a, kk, h)
            if h:
                begun.add(a)

        def finish(a, h):
            lo = wide * a + leaf_n * h
            rest = jnp.where(rowi + j0 == coli + lo, 1.0, 0.0)
            if a:
                rest = rest - pmat[:, lo : lo + leaf_n]
            if h:
                rest = rest - dot_nt(pmat[:, lo - leaf_n : lo], low_of(a))
            pmat[:, lo : lo + leaf_n] = dot_nt(rest, inv_of(a, h))

        def out_at(src_y, h):
            return out.at[pl.ds(pl.multiple_of(share * src_y, 8), share), leaf_cols(h)]

        def out_copy(a, h, src_y, yy):
            return pltpu.make_async_remote_copy(
                src_ref=zmat.at[:, leaf_cols(2 * a + h)], dst_ref=out_at(src_y, h),
                send_sem=out_send.at[2 * a + h], recv_sem=out_recv.at[src_y, h],
                device_id={"row": row, "col": yy}, device_id_type=MESH)

        def ship(a, h, wait):
            @pl.when(y == a)
            def _():
                c = pltpu.make_async_copy(zmat.at[:, leaf_cols(2 * a + h)], out_at(y, h), out_send.at[2 * a + h])
                c.wait() if wait else c.start()

            @pl.when(y != a)
            def _():
                c = out_copy(a, h, y, a)
                c.wait_send() if wait else c.start()

        def backward(a):
            def rest(h):
                r = pmat[:, leaf_cols(2 * a + h)]
                for b in range(a + 1, SIDE):
                    blk = off_of(b, a)[:, leaf_n * h : leaf_n * (h + 1)]
                    r = r - dot_nn(zmat[:, wide * b : wide * (b + 1)], blk)
                return r

            z1 = dot_nn(rest(1), inv_of(a, 1))
            zmat[:, leaf_cols(2 * a + 1)] = z1
            ship(a, 1, False)
            zmat[:, leaf_cols(2 * a)] = dot_nn(rest(0) - dot_nn(z1, low_of(a)), inv_of(a, 0))
            ship(a, 0, False)

        with jax.named_scope("scatter_send"):
            for a in (1, 2):
                scatter_off(a, 0)

            @pl.when((x == y) & (k == 1))
            def _():
                for c in range(3):
                    for r in range(3):
                        low[3 * c + r] = own[part * r : part * (r + 1), part * c : part * (c + 1)]

            for a in range(SIDE):
                scatter_low(a)

        with jax.named_scope("leaf"):
            @pl.when((x == y) & (k == 0))
            def _():
                leaf[...] = own[:, :leaf_n]

            @pl.when((x == y) & (k == 1))
            def _():
                leaf[...] = own[:, leaf_n:]

            @pl.when(x == y)
            def _():
                leaf_inverse(leaf, inv)

            for a in range(SIDE):
                scatter_inv(a)

        def step(name, fn, *args):
            with jax.named_scope(name):
                fn(*args)

        def arrive(rnd):
            if rnd == 1:
                landed_diag()
            elif rnd in HEADS:
                lo, hi, part = HEADS[rnd]
                if lo == 0:
                    landed_off(1, (0,), part)
                if hi == 3:
                    landed_off(2, (0, 1), part)
            else:
                landed_off(3, (rnd - 3,), 2)

        def scatter_rest(q):
            for a in (1, 2):
                scatter_off(a, 1, 8 * q, 8 * (q + 1))

        stages = {"A": stage_a, "B": stage_b, "C": stage_c, "D": stage_d, "P": pair_done, "G": subtract_one, "H": subtract_both, "I": finish,
                  "S": lambda q: scatter_off(3, 2, SIDE * q, SIDE * (q + 1)), "T": scatter_rest}
        for token in ORDER:
            step(token, stages[token[0]], *(int(d) for d in token[1:]))
        for a in range(SIDE - 1, -1, -1):
            step(f"backward{a}", backward, a)

        for rnd in range(ROUNDS):
            sent(strips(rnd, SIDE * SIDE - 1), ring_send.at[rnd])
            sent(strips(rnd, SIDE * SIDE), pair_send.at[rnd])
        others = SIDE * SIDE - 1
        for p in range(2):
            @pl.when((y < x) & (x < 3))
            def _():
                sent(off.at[0, 0 : PARTS[p][1] * others, :], scat_send.at[p])

        @pl.when((y < x) & (x == 3))
        def _():
            sent(off.at[0, 0 : strip * others, :], scat_send.at[0])

        @pl.when(x == y)
        def _():
            sent(inv.at[:, 0 : 8 * others, :], scat_send.at[0])

        for core in range(2):
            @pl.when((x == y) & (k == 1) & (x // 2 == core))
            def _():
                sent(low.at[:, 0 : 8 * (others + 1 - core), :], scat_send.at[1])
        for a in range(SIDE):
            for h in range(2):
                ship(a, h, True)
        for yy in range(SIDE):
            @pl.when(y != yy)
            def _():
                for h in range(2):
                    out_copy(0, h, yy, y).wait_recv()

    return kernel


def solution(mesh):
    count_c = mesh.shape["col"]

    def local_fn(block):
        leaf_n, wide = block.shape
        share = leaf_n // count_c
        strip = leaf_n // (SIDE * SIDE)
        order = wide * count_c
        f32 = jnp.float32
        return pl.pallas_call(
            make_kernel(leaf_n, share, strip),
            out_shape=jax.ShapeDtypeStruct(block.shape, f32),
            in_specs=[pl.BlockSpec(memory_space=pltpu.VMEM)],
            out_specs=pl.BlockSpec(memory_space=pl.ANY),
            scratch_shapes=[
                pltpu.VMEM((6, wide, wide), f32),
                pltpu.VMEM((2, 42, leaf_n // 3, leaf_n // 3), f32),
                pltpu.VMEM((leaf_n, leaf_n), f32),
                pltpu.VMEM((6, leaf_n // 3, leaf_n // 3), f32),
                pltpu.VMEM((9, leaf_n // 3, leaf_n // 3), f32),
                pltpu.VMEM((share, order), f32),
                pltpu.VMEM((share, order), f32),
                pltpu.SemaphoreType.DMA((2,)),
                pltpu.SemaphoreType.DMA((15,)),
                pltpu.SemaphoreType.DMA((ROUNDS,)),
                pltpu.SemaphoreType.DMA((ROUNDS, 15)),
                pltpu.SemaphoreType.DMA((ROUNDS,)),
                pltpu.SemaphoreType.DMA((ROUNDS,)),
                pltpu.SemaphoreType.DMA((2 * SIDE,)),
                pltpu.SemaphoreType.DMA((SIDE, 2)),
            ],
            compiler_params=pltpu.CompilerParams(
                collective_id=0, has_side_effects=True, vmem_limit_bytes=60 * 2**20),
            name="spd_inverse",
        )(block)

    spec = P(("batch", "row"), "col")
    return jax.shard_map(local_fn, mesh=mesh, in_specs=(spec,), out_specs=spec, check_vma=False)
```

```python
import jax
import jax.numpy as jnp
from jax import lax
from jax.experimental import pallas as pl
from jax.experimental.pallas import tpu as pltpu
from jax.sharding import PartitionSpec as P

HIGHEST = lax.Precision.HIGHEST
MESH = pl.DeviceIdType.MESH
SIDE = 4
ROUNDS = 7
ORDER = (
    "A0", "T0", "B00", "B01", "T1", "C00", "C01", "A1", "A2", "C03", "A6", "B02", "C02", "C05",
    "C04", "D00", "B10", "B11", "S0", "C11", "B20", "B21", "C21", "D01", "C10", "B60", "B61", "S1",
    "C20", "C61", "B22", "C60", "C06", "C07", "B12", "S2", "D02", "B62", "C13", "C12", "C15", "C23",
    "C25", "C14", "S3", "C22", "C63", "C24", "C65", "C27", "D10", "D03", "C62", "C64", "C17", "D20",
    "C26", "A4", "C67", "D60", "D11", "D21", "C16", "A5", "D61", "B40", "B41", "C66", "D23", "D12",
    "B50", "B51", "A3", "D13", "D22", "C41", "B42", "P1", "I00", "D63", "D62", "I01", "C51", "C40",
    "P0", "P2", "G100", "B52", "C50", "B30", "C43", "G101", "B31", "C42", "C44", "C45", "I10", "C52",
    "C53", "I11", "C54", "C55", "C31", "C30", "P6", "G200", "C46", "C47", "G201", "C56", "C57", "B32",
    "D40", "G210", "D50", "C32", "C33", "D41", "G211", "D51", "C34", "C35", "I20", "D42", "D43", "I21",
    "D52", "D53", "D30", "C37", "P4", "G310", "C36", "D31", "D32", "G311", "P5", "D33", "H32", "P3",
    "H30", "I30", "I31",
)


def dot_nn(a, b):
    return lax.dot_general(a, b, (((1,), (0,)), ((), ())), precision=HIGHEST, preferred_element_type=jnp.float32)


def dot_nt(a, b):
    return lax.dot_general(a, b, (((1,), (1,)), ((), ())), precision=HIGHEST, preferred_element_type=jnp.float32)


def leaf_inverse(leaf, inv):
    order = leaf.shape[0]
    part = 128
    count = order // part
    rows = lax.broadcasted_iota(jnp.int32, (part, part), 0)
    cols = lax.broadcasted_iota(jnp.int32, (part, part), 1)

    def blk(i, j):
        return leaf[part * i : part * (i + 1), part * j : part * (j + 1)]

    diag = [blk(q, q) for q in range(count)]
    done = [jnp.where(rows == cols, 1.0 / d, 0.0) for d in diag]

    def merge(level, xs):
        rbit, cbit = rows >> level, cols >> level
        low = (rbit == cbit + 1) & (cbit & 1 == 0)
        prods = [dot_nn(jnp.where(low, blk(q, q), 0.0), x) for q, x in enumerate(xs)]
        return tuple(x - dot_nn(x, t) for x, t in zip(xs, prods))

    done = lax.fori_loop(0, part.bit_length() - 1, merge, tuple(done))
    out = {}
    for i in range(count):
        out[i, i] = done[i]
    for gap in range(1, count):
        for j in range(count - gap):
            i = j + gap
            acc = dot_nn(blk(i, j), out[j, j])
            for k in range(j + 1, i):
                acc = acc + dot_nn(blk(i, k), out[k, j])
            out[i, j] = -dot_nn(out[i, i], acc)
    for n, (i, j) in enumerate((i, j) for j in range(count) for i in range(j, count)):
        inv[n] = out[i, j]


def make_kernel(leaf_n, share, strip):
    wide = 2 * leaf_n
    part = leaf_n // 3
    head = 8
    shifts = (0, SIDE - 1, 1, 2)
    DIRS = (1, -1, 1, -1)

    def kernel(block, out, own, off, diag, leaf, inv, low, pmat, zmat,
               scat_send, scat_recv, ring_send, ring_recv, pair_send, pair_recv, out_send, out_recv, load_sem):
        row = lax.axis_index("row")
        y = lax.axis_index("col")
        x = row // 2
        k = row % 2
        me = SIDE * x + y
        def off_of(a, yy):
            return off.at[a * (a - 1) // 2 + yy]

        def dev(cx, cy, core):
            return {"row": 2 * cx + core, "col": cy}

        load = pltpu.make_async_copy(block, own, load_sem.at[0])
        load.start()

        barrier = pltpu.get_barrier_semaphore()

        def greet(t, carry):
            @pl.when(t != row * SIDE + y)
            def _():
                pl.semaphore_signal(barrier, inc=1, device_id={"row": t // SIDE, "col": t % SIDE}, device_id_type=MESH)
            return carry

        lax.fori_loop(0, 2 * SIDE * SIDE, greet, 0)
        load.wait()
        pl.semaphore_wait(barrier, 2 * SIDE * SIDE - 1)

        def scatter(src_of, dst_of, cond, core, send_row, sem, first=0, last=SIDE * SIDE):
            @pl.when(cond)
            def _():
                def body(m, carry):
                    src, dst = src_of(m), dst_of(m)
                    here = (m == me) & (core == k)

                    @pl.when(here)
                    def _():
                        pltpu.make_async_copy(src, dst, scat_recv.at[sem]).start()

                    @pl.when(jnp.logical_not(here))
                    def _():
                        pltpu.make_async_remote_copy(
                            src_ref=src, dst_ref=dst, send_sem=scat_send.at[send_row], recv_sem=scat_recv.at[sem],
                            device_id=dev(m // SIDE, m % SIDE, core), device_id_type=MESH).start()
                    return carry

                lax.fori_loop(first, last, body, 0)

        PARTS = {0: (0, head), 1: (head, strip - head), 2: (0, strip)}

        def strip_rows(m, core, part):
            start, count = PARTS[part]
            return pl.ds(pl.multiple_of(leaf_n * core + strip * m, 8) + start, count)

        def off_src(part):
            return lambda m: own.at[strip_rows(m, 0, part), :]

        def off_dst(a, yy, part):
            return lambda m: off_of(a, yy).at[strip_rows(m, k, part), :]

        def off_sem(a, yy, part):
            return {1: 0, 2: 1 + yy, 3: 6 + yy}[a] + (3 if part == 1 else 0)

        def scatter_off(a, part, *span):
            for yy in range(a):
                scatter(off_src(part), off_dst(a, yy, part), (x == a) & (y == yy), k, part % 2, off_sem(a, yy, part),
                        *span)

        def band(m):
            return pl.ds(pl.multiple_of(8 * m, 8), 8)

        def low_at(a):
            return 6 * SIDE + 9 * (a % 2)

        def scatter_low(a):
            core = a // 2
            scatter(lambda m: low.at[:, band(m), :], lambda m: diag.at[core, low_at(a) : low_at(a) + 9, band(m), :],
                    (x == a) & (y == a) & (k == 1), core, 1, 13 + a % 2)

        def scatter_inv(a):
            scatter(lambda m: inv.at[:, band(m), :], lambda m: diag.at[k, 6 * a : 6 * (a + 1), band(m), :],
                    (x == a) & (y == a), k, 0, 9 + a)

        def landed(dst, src_like, sem, is_source):
            @pl.when(is_source)
            def _():
                pltpu.make_async_copy(src_like, dst, scat_recv.at[sem]).wait()

            @pl.when(jnp.logical_not(is_source))
            def _():
                pltpu.make_async_remote_copy(
                    src_ref=src_like, dst_ref=dst, send_sem=scat_send.at[0], recv_sem=scat_recv.at[sem],
                    device_id=dev(x, y, 1 - k), device_id_type=MESH).wait_recv()

        def landed_off(a, places, part):
            for yy in places:
                landed(off_dst(a, yy, part)(me), off_src(part)(me), off_sem(a, yy, part), (x == a) & (y == yy))

        def landed_diag():
            for a in range(SIDE):
                landed(diag.at[k, 6 * a : 6 * (a + 1), band(me), :], inv.at[:, band(me), :], 9 + a, (x == a) & (y == a))
            for q in range(2):
                a = 2 * k + q
                landed(diag.at[k, low_at(q) : low_at(q) + 9, band(me), :], low.at[:, band(me), :], 13 + q,
                       (x == a) & (y == a) & (k == 1))

        def relative(du, dv):
            cx = (x + du + k * (dv - du)) % SIDE
            cy = (y + dv + k * (du - dv)) % SIDE
            return cx, cy, SIDE * cx + cy

        chips = {(du, dv): relative(du, dv) for du in range(SIDE) for dv in range(SIDE)}

        def chip_at(du, dv):
            return chips[du % SIDE, dv % SIDE]

        HEADS = {0: (0, 3, 0), 2: (0, 1, 1), 6: (1, 3, 1)}

        def piece(rnd, core, chip):
            m = chip[2]
            if rnd == 1:
                return diag.at[core, :, band(m), :]
            if rnd in HEADS:
                lo, hi, part = HEADS[rnd]
                return off.at[lo:hi, strip_rows(m, core, part), :]
            return off.at[rnd, strip_rows(m, core, 2), :]

        def strips(rnd, n):
            if rnd == 1:
                return diag.at[0, :, 0 : 8 * n, :]
            if rnd in HEADS:
                lo, hi, part = HEADS[rnd]
                return off.at[lo:hi, 0 : PARTS[part][1] * n, :]
            return off.at[rnd, 0 : strip * n, :]

        def sent(ref, sem):
            pltpu.make_async_remote_copy(
                src_ref=ref, dst_ref=ref, send_sem=sem, recv_sem=scat_recv.at[0],
                device_id=dev(x, y, 1 - k), device_id_type=MESH).wait_send()

        def ring_copy(rnd, du, dv, tu, tv, idx):
            ref = piece(rnd, k, chip_at(du, dv))
            return pltpu.make_async_remote_copy(
                src_ref=ref, dst_ref=ref, send_sem=ring_send.at[rnd], recv_sem=ring_recv.at[rnd, idx],
                device_id=dev(*chip_at(tu, tv)[:2], k), device_id_type=MESH)

        def ring_start(*args):
            ring_copy(*args).start()

        def ring_wait(rnd, du, dv, idx):
            ring_copy(rnd, du, dv, 0, 1, idx).wait_recv()

        def pair_start(rnd, g, dv):
            ref = piece(rnd, k, chip_at(shifts[g], dv))
            pltpu.make_async_remote_copy(
                src_ref=ref, dst_ref=ref, send_sem=pair_send.at[rnd], recv_sem=pair_recv.at[rnd],
                device_id=dev(x, y, 1 - k), device_id_type=MESH).start()

        def spread(rnd, g):
            ring_start(rnd, shifts[g], 0, 0, 1, 3 + 3 * g)
            ring_start(rnd, shifts[g], 0, 0, -1, 4 + 3 * g)
            pair_start(rnd, g, 0)

        def stage_a(rnd):
            arrive(rnd)
            ring_start(rnd, 0, 0, 1, 0, 0)
            ring_start(rnd, 0, 0, -1, 0, 1)
            spread(rnd, 0)

        def stage_b(rnd, j):
            ring_wait(rnd, (-1, 1, 2)[j], 0, j)
            if j == 0 and rnd % 2 == 0:
                ring_start(rnd, -1, 0, 1, 0, 2)
            if j == 1 and rnd % 2 == 1:
                ring_start(rnd, 1, 0, -1, 0, 2)
            spread(rnd, j + 1)

        def stage_c(rnd, j):
            g, back = j // 2, j % 2
            from_v = 1 if back else -1
            ring_wait(rnd, shifts[g], from_v, 3 + 3 * g + back)
            if DIRS[g] == -from_v:
                ring_start(rnd, shifts[g], from_v, 0, -from_v, 5 + 3 * g)
            pair_start(rnd, g, from_v)

        def stage_d(rnd, g):
            ring_wait(rnd, shifts[g], 2, 5 + 3 * g)
            pair_start(rnd, g, 2)

        def pair_done(rnd):
            ref = strips(rnd, SIDE * SIDE)
            pltpu.make_async_remote_copy(
                src_ref=ref, dst_ref=ref, send_sem=pair_send.at[rnd], recv_sem=pair_recv.at[rnd],
                device_id=dev(x, y, 1 - k), device_id_type=MESH).wait_recv()

        def column(core, start, count):
            col = diag[core, pl.ds(start, count)].reshape(part * count, part)
            return col if count == 3 else jnp.concatenate([jnp.zeros((part * (3 - count), part), jnp.float32), col], axis=0)

        def low_of(a):
            return jnp.concatenate([column(a // 2, low_at(a) + 3 * c, 3) for c in range(3)], axis=1)

        def inv_of(a, h):
            return jnp.concatenate([column(h, 6 * a + n, c) for n, c in ((0, 3), (3, 2), (5, 1))], axis=1)

        j0 = leaf_n * row + share * y
        rowi = lax.broadcasted_iota(jnp.int32, (share, leaf_n), 0)
        coli = lax.broadcasted_iota(jnp.int32, (share, leaf_n), 1)

        def leaf_cols(i):
            return pl.ds(pl.multiple_of(leaf_n * i, 128), leaf_n)

        begun = set()

        def subtract(a, kk, h):
            place = leaf_cols(2 * a + h)
            rows = pl.ds(pl.multiple_of(leaf_n * h, 8), leaf_n)
            acc = dot_nt(pmat[:, wide * kk : wide * (kk + 1)], off_of(a, kk)[rows, :])
            pmat[:, place] = pmat[:, place] + acc if a in begun else acc

        def subtract_both(a, kk):
            def body(h, carry):
                subtract(a, kk, h)
                return carry

            lax.fori_loop(0, 2, body, 0)
            begun.add(a)

        def subtract_one(a, kk, h):
            subtract(a, kk, h)
            if h:
                begun.add(a)

        def finish(a, h):
            lo = wide * a + leaf_n * h
            rest = jnp.where(rowi + j0 == coli + lo, 1.0, 0.0)
            if a:
                rest = rest - pmat[:, lo : lo + leaf_n]
            if h:
                rest = rest - dot_nt(pmat[:, lo - leaf_n : lo], low_of(a))
            pmat[:, lo : lo + leaf_n] = dot_nt(rest, inv_of(a, h))

        def out_at(src_y, h):
            return out.at[pl.ds(pl.multiple_of(share * src_y, 8), share), leaf_cols(h)]

        def out_copy(a, h, src_y, yy):
            return pltpu.make_async_remote_copy(
                src_ref=zmat.at[:, leaf_cols(2 * a + h)], dst_ref=out_at(src_y, h),
                send_sem=out_send.at[2 * a + h], recv_sem=out_recv.at[src_y, h],
                device_id={"row": row, "col": yy}, device_id_type=MESH)

        def ship(a, h, wait):
            @pl.when(y == a)
            def _():
                c = pltpu.make_async_copy(zmat.at[:, leaf_cols(2 * a + h)], out_at(y, h), out_send.at[2 * a + h])
                c.wait() if wait else c.start()

            @pl.when(y != a)
            def _():
                c = out_copy(a, h, y, a)
                c.wait_send() if wait else c.start()

        def backward(a):
            def rest(h):
                r = pmat[:, leaf_cols(2 * a + h)]
                for b in range(a + 1, SIDE):
                    blk = off_of(b, a)[:, leaf_n * h : leaf_n * (h + 1)]
                    r = r - dot_nn(zmat[:, wide * b : wide * (b + 1)], blk)
                return r

            z1 = dot_nn(rest(1), inv_of(a, 1))
            zmat[:, leaf_cols(2 * a + 1)] = z1
            ship(a, 1, False)
            zmat[:, leaf_cols(2 * a)] = dot_nn(rest(0) - dot_nn(z1, low_of(a)), inv_of(a, 0))
            ship(a, 0, False)

        with jax.named_scope("scatter_send"):
            for a in (1, 2):
                scatter_off(a, 0)

            @pl.when((x == y) & (k == 1))
            def _():
                for c in range(3):
                    for r in range(3):
                        low[3 * c + r] = own[part * r : part * (r + 1), part * c : part * (c + 1)]

            for a in range(SIDE):
                scatter_low(a)

        with jax.named_scope("leaf"):
            @pl.when((x == y) & (k == 0))
            def _():
                leaf[...] = own[:, :leaf_n]

            @pl.when((x == y) & (k == 1))
            def _():
                leaf[...] = own[:, leaf_n:]

            @pl.when(x == y)
            def _():
                leaf_inverse(leaf, inv)

            for a in range(SIDE):
                scatter_inv(a)

        def step(name, fn, *args):
            with jax.named_scope(name):
                fn(*args)

        def arrive(rnd):
            if rnd == 1:
                landed_diag()
            elif rnd in HEADS:
                lo, hi, part = HEADS[rnd]
                if lo == 0:
                    landed_off(1, (0,), part)
                if hi == 3:
                    landed_off(2, (0, 1), part)
            else:
                landed_off(3, (rnd - 3,), 2)

        def scatter_rest(q):
            for a in (1, 2):
                scatter_off(a, 1, 8 * q, 8 * (q + 1))

        stages = {"A": stage_a, "B": stage_b, "C": stage_c, "D": stage_d, "P": pair_done, "G": subtract_one, "H": subtract_both, "I": finish,
                  "S": lambda q: scatter_off(3, 2, SIDE * q, SIDE * (q + 1)), "T": scatter_rest}
        for token in ORDER:
            step(token, stages[token[0]], *(int(d) for d in token[1:]))
        for a in range(SIDE - 1, -1, -1):
            step(f"backward{a}", backward, a)

        for rnd in range(ROUNDS):
            sent(strips(rnd, SIDE * SIDE - 1), ring_send.at[rnd])
            sent(strips(rnd, SIDE * SIDE), pair_send.at[rnd])
        others = SIDE * SIDE - 1
        for p in range(2):
            @pl.when((y < x) & (x < 3))
            def _():
                sent(off.at[0, 0 : PARTS[p][1] * others, :], scat_send.at[p])

        @pl.when((y < x) & (x == 3))
        def _():
            sent(off.at[0, 0 : strip * others, :], scat_send.at[0])

        @pl.when(x == y)
        def _():
            sent(inv.at[:, 0 : 8 * others, :], scat_send.at[0])

        for core in range(2):
            @pl.when((x == y) & (k == 1) & (x // 2 == core))
            def _():
                sent(low.at[:, 0 : 8 * (others + 1 - core), :], scat_send.at[1])
        for a in range(SIDE):
            for h in range(2):
                ship(a, h, True)
        for yy in range(SIDE):
            @pl.when(y != yy)
            def _():
                for h in range(2):
                    out_copy(0, h, yy, y).wait_recv()

    return kernel


def solution(mesh):
    count_c = mesh.shape["col"]

    def local_fn(block):
        leaf_n, wide = block.shape
        share = leaf_n // count_c
        strip = leaf_n // (SIDE * SIDE)
        order = wide * count_c
        f32 = jnp.float32
        return pl.pallas_call(
            make_kernel(leaf_n, share, strip),
            out_shape=jax.ShapeDtypeStruct(block.shape, f32),
            in_specs=[pl.BlockSpec(memory_space=pl.ANY)],
            out_specs=pl.BlockSpec(memory_space=pl.ANY),
            scratch_shapes=[
                pltpu.VMEM(block.shape, f32),
                pltpu.VMEM((6, wide, wide), f32),
                pltpu.VMEM((2, 42, leaf_n // 3, leaf_n // 3), f32),
                pltpu.VMEM((leaf_n, leaf_n), f32),
                pltpu.VMEM((6, leaf_n // 3, leaf_n // 3), f32),
                pltpu.VMEM((9, leaf_n // 3, leaf_n // 3), f32),
                pltpu.VMEM((share, order), f32),
                pltpu.VMEM((share, order), f32),
                pltpu.SemaphoreType.DMA((2,)),
                pltpu.SemaphoreType.DMA((15,)),
                pltpu.SemaphoreType.DMA((ROUNDS,)),
                pltpu.SemaphoreType.DMA((ROUNDS, 15)),
                pltpu.SemaphoreType.DMA((ROUNDS,)),
                pltpu.SemaphoreType.DMA((ROUNDS,)),
                pltpu.SemaphoreType.DMA((2 * SIDE,)),
                pltpu.SemaphoreType.DMA((SIDE, 2)),
                pltpu.SemaphoreType.DMA((1,)),
            ],
            compiler_params=pltpu.CompilerParams(
                collective_id=0, has_side_effects=True, vmem_limit_bytes=60 * 2**20),
            name="spd_inverse",
        )(block)

    spec = P(("batch", "row"), "col")
    return jax.shard_map(local_fn, mesh=mesh, in_specs=(spec,), out_specs=spec, check_vma=False)
```
